32 devices in a mesh: dp: 4 (over y, z), sp: 8 (over x, core).
Axes of the slice: x: 4, y: 2, z: 2, core: 2. Of those that a mesh axis runs over, the one named last changes fastest.
The devices are a block of a 4x4x8 slice.
Arguments:
- images: float32 [24, 224, 224, 3], P('dp', 'sp'), parts along dimension 0
- w_patch: bfloat16 [14, 14, 3, 1152], replicated
- b_patch: float32 [1152], replicated
- pos_embed: bfloat16 [256, 1152], P('sp')
- ln1_gain: float32 [1152], replicated
- ln1_bias: float32 [1152], replicated
- w_qkv: bfloat16 [1152, 3, 16, 72], replicated
- b_qkv: float32 [3, 16, 72], replicated
- w_out: bfloat16 [16, 72, 1152], replicated
- b_out: float32 [1152], replicated
- ln2_gain: float32 [1152], replicated
- ln2_bias: float32 [1152], replicated
- w_fc1: bfloat16 [1152, 4304], replicated
- b_fc1: float32 [4304], replicated
- w_fc2: bfloat16 [4304, 1152], replicated
- b_fc2: float32 [1152], replicated
Outputs:
- output: bfloat16 [24, 256, 1152], P('dp', 'sp'), parts along dimension 0
There are 4 independent parts. The reference program is written for one: setup_inputs(seed, part) draws one part's arguments, and reference() takes and returns one part's arrays. A program takes and returns all parts, laid end to end along the dimension named above; an argument that names none is the same for every part.
All inputs are finite; a program needn't handle non-finite values.
Results may differ from the reference program's by a relative error of at most 0.0126451.
Values are sent between devices in bfloat16 or wider.
A program may use at most 768 MiB of HBM per device.

```python
import jax
import jax.numpy as jnp
from jax import lax

B = 6
IMG = 224
PATCH = 14
D = 1152
HEADS = 16
HEAD = 72
FF = 4304

GRID = IMG // PATCH
TOKENS = GRID * GRID
PATCH_DIM = PATCH * PATCH * 3
LN_EPS = 1e-6


def draw_normal(rng_key, arr_shape, std_dev):
    return jax.random.normal(rng_key, arr_shape, jnp.float32) * std_dev


def smooth_images(base_key, num_images):
    key_freq, key_phase, key_amp, key_noise = jax.random.split(base_key, 4)
    wave_freq = jax.random.uniform(key_freq, (num_images, 8, 2), jnp.float32, -4.0, 4.0) * (2.0 * jnp.pi / IMG)
    wave_phase = jax.random.uniform(key_phase, (num_images, 8, 3), jnp.float32, 0.0, 2.0 * jnp.pi)
    wave_amp = draw_normal(key_amp, (num_images, 8, 3), 0.5)
    coords = jnp.arange(IMG, dtype=jnp.float32)
    row_angle = wave_freq[:, :, 0, None] * coords
    col_angle = wave_freq[:, :, 1, None, None] * coords[:, None] + wave_phase[:, :, None, :]
    waves = (jnp.einsum('nky,nkxc->nyxc', jnp.cos(row_angle), wave_amp[:, :, None, :] * jnp.cos(col_angle))
             - jnp.einsum('nky,nkxc->nyxc', jnp.sin(row_angle), wave_amp[:, :, None, :] * jnp.sin(col_angle)))
    return waves + draw_normal(key_noise, (num_images, IMG, IMG, 3), 0.2)


def setup_inputs(seed: int = 0, part: int = 0) -> dict:
    sub_keys = jax.random.split(jax.random.key(seed), 16)
    qk_gain = jnp.array([1.5, 1.5, 1.0], jnp.float32)[None, :, None, None]
    return {
        'images': smooth_images(jax.random.fold_in(sub_keys[0], part), B),
        'w_patch': draw_normal(sub_keys[1], (PATCH, PATCH, 3, D), PATCH_DIM ** -0.5).astype(jnp.bfloat16),
        'b_patch': draw_normal(sub_keys[2], (D,), 0.5),
        'pos_embed': draw_normal(sub_keys[3], (TOKENS, D), 1.0).astype(jnp.bfloat16),
        'ln1_gain': 1.0 + draw_normal(sub_keys[4], (D,), 0.2),
        'ln1_bias': draw_normal(sub_keys[5], (D,), 0.5),
        'w_qkv': (draw_normal(sub_keys[6], (D, 3, HEADS, HEAD), D ** -0.5) * qk_gain).astype(jnp.bfloat16),
        'b_qkv': draw_normal(sub_keys[7], (3, HEADS, HEAD), 0.5),
        'w_out': draw_normal(sub_keys[8], (HEADS, HEAD, D), 2.0 * D ** -0.5).astype(jnp.bfloat16),
        'b_out': draw_normal(sub_keys[9], (D,), 0.5),
        'ln2_gain': 1.0 + draw_normal(sub_keys[10], (D,), 0.2),
        'ln2_bias': draw_normal(sub_keys[11], (D,), 0.5),
        'w_fc1': draw_normal(sub_keys[12], (D, FF), D ** -0.5).astype(jnp.bfloat16),
        'b_fc1': draw_normal(sub_keys[13], (FF,), 0.5),
        'w_fc2': draw_normal(sub_keys[14], (FF, D), 1.5 * FF ** -0.5).astype(jnp.bfloat16),
        'b_fc2': draw_normal(sub_keys[15], (D,), 0.5),
    }


def layer_norm(x_in, ln_gain, ln_bias):
    row_mean = jnp.mean(x_in, axis=-1, keepdims=True)
    centered = x_in - row_mean
    variance = jnp.mean(centered * centered, axis=-1, keepdims=True)
    return centered * lax.rsqrt(variance + LN_EPS) * ln_gain + ln_bias


def reference(images, w_patch, b_patch, pos_embed, ln1_gain, ln1_bias, w_qkv, b_qkv, w_out, b_out, ln2_gain, ln2_bias, w_fc1, b_fc1, w_fc2, b_fc2):
    w_patch_flat = w_patch.reshape(PATCH_DIM, D)
    w_qkv_flat = w_qkv.reshape(D, 3 * D)
    b_qkv_flat = b_qkv.reshape(3 * D)
    w_out_flat = w_out.reshape(D, D)
    pos_f32 = pos_embed.astype(jnp.float32)

    def encode_image(single_image):
        pixels = single_image.astype(jnp.bfloat16).reshape(GRID, PATCH, GRID, PATCH, 3)
        patches = jnp.transpose(pixels, (0, 2, 1, 3, 4)).reshape(TOKENS, PATCH_DIM)
        patch_embed = jnp.dot(patches, w_patch_flat, preferred_element_type=jnp.float32)
        x_zero = (patch_embed + b_patch + pos_f32).astype(jnp.bfloat16)
        normed = layer_norm(x_zero.astype(jnp.float32), ln1_gain, ln1_bias).astype(jnp.bfloat16)
        qkv_proj = (jnp.dot(normed, w_qkv_flat, preferred_element_type=jnp.float32) + b_qkv_flat).astype(jnp.bfloat16)
        queries = qkv_proj[:, :D].reshape(GRID, GRID, HEADS, HEAD)
        keys_all = qkv_proj[:, D:2 * D].reshape(TOKENS, HEADS, HEAD).astype(jnp.float32)
        values_all = qkv_proj[:, 2 * D:].reshape(TOKENS, HEADS, HEAD).astype(jnp.float32)

        def attend_row(row_queries):
            scores = jnp.einsum('qhe,khe->hqk', row_queries.astype(jnp.float32), keys_all) * HEAD ** -0.5
            weights = jax.nn.softmax(scores, axis=-1).astype(jnp.bfloat16).astype(jnp.float32)
            return jnp.einsum('hqk,khe->qhe', weights, values_all).astype(jnp.bfloat16)

        attended = lax.map(attend_row, queries).reshape(TOKENS, D)
        residual = x_zero.astype(jnp.float32) + jnp.dot(attended, w_out_flat, preferred_element_type=jnp.float32) + b_out
        normed_two = layer_norm(residual, ln2_gain, ln2_bias).astype(jnp.bfloat16)
        hidden = jax.nn.gelu(jnp.dot(normed_two, w_fc1, preferred_element_type=jnp.float32) + b_fc1, approximate=True).astype(jnp.bfloat16)
        return (residual + jnp.dot(hidden, w_fc2, preferred_element_type=jnp.float32) + b_fc2).astype(jnp.bfloat16)

    return lax.map(encode_image, images)
```

```python
import functools
import math

import jax
import jax.numpy as jnp
from jax import lax
from jax.experimental import pallas as pl
from jax.experimental.pallas import tpu as pltpu
from jax.sharding import PartitionSpec as P

LN_EPS = 1e-6
F32 = jnp.float32
BF16 = jnp.bfloat16
NT = (((1,), (1,)), ((), ()))
NN = (((1,), (0,)), ((), ()))


def dot(a, b, dims=NN):
    return lax.dot_general(a, b, dims, preferred_element_type=F32)


def norm(z, gain, bias):
    mean = jnp.mean(z, axis=-1, keepdims=True)
    cen = z - mean
    var = jnp.mean(cen * cen, axis=-1, keepdims=True)
    return cen * lax.rsqrt(var + LN_EPS) * gain + bias


def gelu(x):
    inner = math.sqrt(2.0 / math.pi) * (x + 0.044715 * (x * x * x))
    return 0.5 * x * (1.0 + jnp.tanh(inner))


def chunk_transpose(w, chunk):
    rows, lanes = w.shape
    r = lax.broadcasted_iota(jnp.int32, w.shape, 0) % 8
    c = lax.broadcasted_iota(jnp.int32, w.shape, 1) // chunk
    for s in (4, 2, 1):
        up = pltpu.roll(pltpu.roll(w, s * chunk, 1), rows - s, 0)
        down = pltpu.roll(pltpu.roll(w, lanes - s * chunk, 1), s, 0)
        rb, cb = (r & s) != 0, (c & s) != 0
        w = jnp.where(rb == cb, w, jnp.where(cb, up, down))
    return w


def body(cfg, img_hbm, wp_hbm, bp, pos, g1, be1, wqkv_hbm, bqkv, wo_hbm, bo, g2, be2, w1_hbm, b1, w2_hbm, b2, out,
         img, wp_raw, wp, wqkv, wo, w1, w2, zf, xs, x0, y1, yrecv, kall, qt, vt, ot, osend, orecv, res, y2, acc, kbias,
         wsem, ssem, rsem, ossem, orsem):
    n, nimg, tok, d, heads, hd, ff, patch, chans = cfg
    ntok = n * tok
    per, own = 4, 3
    me = lax.axis_index('sp')
    half = nimg // 2

    def owner(i):
        return per * (i // own) + i % own

    cp_img = [pltpu.make_async_copy(img_hbm.at[pl.ds(half * k, half)], img.at[pl.ds(half * k, half)], wsem.at[k]) for k in range(2)]
    cp_wp = pltpu.make_async_copy(wp_hbm, wp_raw, wsem.at[2])
    cp_wqkv = pltpu.make_async_copy(wqkv_hbm, wqkv, wsem.at[3])
    cp_wo = pltpu.make_async_copy(wo_hbm, wo, wsem.at[4])
    cp_w1 = pltpu.make_async_copy(w1_hbm, w1, wsem.at[5])
    cp_w2 = pltpu.make_async_copy(w2_hbm, w2, wsem.at[6])
    cp_img[0].start()
    cp_img[1].start()
    cp_wp.start()
    barrier = pltpu.get_barrier_semaphore()
    for k in range(1, n):
        pl.semaphore_signal(barrier, inc=1, device_id={'sp': lax.rem(me + k, n)}, device_id_type=pl.DeviceIdType.MESH)

    zf[...] = jnp.zeros_like(zf)
    lrow = lax.broadcasted_iota(jnp.int32, (224, 256), 0)
    lcol = lax.broadcasted_iota(jnp.int32, (224, 256), 1)
    sel = jnp.where((lcol % 16 < patch) & (lrow == patch * (lcol // 16) + lcol % 16), 1.0, 0.0).astype(BF16)
    wp[...] = jnp.zeros_like(wp)

    rows_half = half * tok
    for k in range(2):
        cp_img[k].wait()
        if k == 0:
            cp_wqkv.start()
            cp_wo.start()
            cp_w1.start()
            cp_w2.start()
        for b in range(half):
            for y in range(2):
                for c in range(chans):
                    zf[(b * 2 + y) * chans + c, 0:patch, :] = img[half * k + b, c, patch * y:patch * y + patch, :]
        nz = half * 2 * chans
        u = dot(zf[...].reshape(nz * 16, 224).astype(BF16), sel)
        u = u.reshape(nz, 2, 8, 256)
        for ph in range(2):
            parts = []
            for xh in range(2):
                blk = u[:, ph, :, 128 * xh:128 * xh + 128].reshape(nz * 8, 128)
                parts.append(chunk_transpose(blk, 16).reshape(nz, 1, 8, 128))
            t = jnp.concatenate(parts, axis=1).reshape(half * 2, chans, 16, 128).astype(BF16)
            for c in range(chans):
                xs[pl.ds(rows_half * k, rows_half), 256 * c + 128 * ph:256 * c + 128 * ph + 128] = t[:, c].reshape(rows_half, 128)
        if k == 0:
            cp_wp.wait()
            for c in range(chans):
                for p in range(patch):
                    wp[c * 16 + p, 0:patch, :] = wp_raw[p * chans + c]
        e = dot(xs[pl.ds(rows_half * k, rows_half), :], wp[...].reshape(chans * 256, d))
        base = bp[...] + pos[...].astype(F32)
        e = e + jnp.concatenate([base] * half, axis=0)
        xb = e.astype(BF16)
        x0[pl.ds(rows_half * k, rows_half), :] = xb
        y1[pl.ds(rows_half * k, rows_half), :] = norm(xb.astype(F32), g1[...], be1[...]).astype(BF16)
        if k == 0:
            pl.semaphore_wait(barrier, n - 1)
        for i in range(half * k, half * k + half):
            o = owner(i)

            @pl.when(me != o)
            def _():
                pltpu.make_async_remote_copy(
                    y1.at[pl.ds(tok * i, tok)], yrecv.at[pl.ds(pl.multiple_of(tok * me, tok), tok)],
                    ssem.at[i], rsem.at[me], device_id={'sp': o}, device_id_type=pl.DeviceIdType.MESH).start()

            @pl.when(me == o)
            def _():
                yrecv[pl.ds(pl.multiple_of(tok * me, tok), tok), :] = y1[tok * i:tok * i + tok, :]

    img_idx = own * (me // per) + lax.rem(me, per)

    @pl.when(lax.rem(me, per) < own)
    def _():
        for k in range(1, n):
            s = lax.rem(me + k, n)
            pltpu.make_async_remote_copy(
                y1.at[pl.ds(0, tok)], yrecv.at[pl.ds(pl.multiple_of(tok * s, tok), tok)],
                ssem.at[0], rsem.at[s], device_id={'sp': s}, device_id_type=pl.DeviceIdType.MESH).wait_recv()
        cp_wqkv.wait()
        y = yrecv[...]
        for h in range(heads):
            kbias[0:1, hd * h:hd * h + hd] = bqkv[1, h:h + 1, :]
        for j in range(0, d, 256):
            w = min(256, d - j)
            kall[:, j:j + w] = (dot(y, wqkv[d + j:d + j + w, :], NT) + kbias[0:1, j:j + w]).astype(BF16)
        qbt = jnp.transpose(bqkv[0])
        vbt = jnp.transpose(bqkv[2])
        hh = heads // 2
        for a in range(2):
            qt[pl.ds(hd * hh * a, hd * hh), :] = dot(wqkv[hd * hh * a:hd * hh * a + hd * hh, :], y, NT)
            vt[pl.ds(hd * hh * a, hd * hh), :] = dot(wqkv[2 * d + hd * hh * a:2 * d + hd * hh * a + hd * hh, :], y, NT)
        scale = hd ** -0.5
        for h in range(heads):
            win = min(hd * h // 128 * 128, d - 256)
            off = hd * h - win
            q = qt[hd * h:hd * h + hd, :] + qbt[:, h:h + 1]
            pads = [jnp.zeros((k, ntok), F32) if k else None for k in (off, 256 - off - hd)]
            q = jnp.concatenate([z for z in (pads[0], q, pads[1]) if z is not None], axis=0).astype(BF16)
            s = dot(kall[:, win:win + 256], q) * scale
            m = jnp.max(s, axis=0, keepdims=True)
            p = jnp.exp(s - m)
            p = (p * (1.0 / jnp.sum(p, axis=0, keepdims=True))).astype(BF16)
            v = (vt[hd * h:hd * h + hd, :] + vbt[:, h:h + 1]).astype(BF16)
            ot[pl.ds(hd * h, hd), :] = dot(v, p)
        eye = jnp.where(lax.broadcasted_iota(jnp.int32, (ntok, ntok), 0) == lax.broadcasted_iota(jnp.int32, (ntok, ntok), 1),
                        1.0, 0.0).astype(BF16)
        for j in range(0, d, 256):
            w = min(256, d - j)
            osend[:, j:j + w] = dot(eye, ot[j:j + w, :].astype(BF16), NT).astype(BF16)
        for k in (4, 5, 3, 2, 6, 7, 1):
            s = lax.rem(me + k, n)
            pltpu.make_async_remote_copy(
                osend.at[pl.ds(pl.multiple_of(tok * s, tok), tok)], orecv.at[pl.ds(pl.multiple_of(tok * img_idx, tok), tok)],
                ossem.at[s], orsem.at[img_idx], device_id={'sp': s}, device_id_type=pl.DeviceIdType.MESH).start()
        orecv[pl.ds(pl.multiple_of(tok * img_idx, tok), tok), :] = osend[pl.ds(pl.multiple_of(tok * me, tok), tok), :]

    @pl.when(lax.rem(me, per) >= own)
    def _():
        cp_wqkv.wait()

    for i in range(nimg):
        o = owner(i)

        @pl.when(me != o)
        def _():
            pltpu.make_async_remote_copy(
                osend.at[pl.ds(0, tok)], orecv.at[pl.ds(tok * i, tok)],
                ossem.at[0], orsem.at[i], device_id={'sp': o}, device_id_type=pl.DeviceIdType.MESH).wait_recv()

    cp_wo.wait()
    r = x0[...].astype(F32) + dot(orecv[...], wo[...]) + bo[...]
    res[...] = r
    y2[...] = norm(r, g2[...], be2[...]).astype(BF16)
    cp_w1.wait()
    cp_w2.wait()
    step = 512
    full = ff // step
    acc[...] = jnp.zeros_like(acc)

    def mlp(start, size):
        h = dot(y2[...], w1[pl.ds(start, size), :], NT) + b1[:, pl.ds(start, size)]
        acc[...] += dot(gelu(h).astype(BF16), w2[pl.ds(start, size), :])

    def mlp_step(c, carry):
        mlp(pl.multiple_of(c * step, step), step)
        return carry

    lax.fori_loop(0, full, mlp_step, 0)
    mlp(full * step, ff - full * step)
    out[...] = (res[...] + acc[...] + b2[...]).astype(BF16)

    for i in range(nimg):
        o = owner(i)

        @pl.when(me != o)
        def _():
            pltpu.make_async_remote_copy(
                y1.at[pl.ds(tok * i, tok)], yrecv.at[pl.ds(0, tok)],
                ssem.at[i], rsem.at[0], device_id={'sp': o}, device_id_type=pl.DeviceIdType.MESH).wait_send()

    @pl.when(lax.rem(me, per) < own)
    def _():
        for k in range(1, n):
            s = lax.rem(me + k, n)
            pltpu.make_async_remote_copy(
                osend.at[pl.ds(0, tok)], orecv.at[pl.ds(0, tok)],
                ossem.at[s], orsem.at[0], device_id={'sp': s}, device_id_type=pl.DeviceIdType.MESH).wait_send()


def solution(mesh):
    n = mesh.shape['sp']

    def device_step(images, w_patch, b_patch, pos_embed, ln1_gain, ln1_bias, w_qkv, b_qkv, w_out, b_out, ln2_gain, ln2_bias, w_fc1, b_fc1, w_fc2, b_fc2):
        nimg, rows, width, chans = images.shape
        tok, d = pos_embed.shape
        patch = w_patch.shape[0]
        _, _, heads, hd = w_qkv.shape
        ff = w_fc1.shape[1]
        m = nimg * tok
        cfg = (n, nimg, tok, d, heads, hd, ff, patch, chans)
        img_t = jnp.transpose(images, (0, 3, 1, 2))
        wp_t = jnp.transpose(w_patch, (0, 2, 1, 3)).reshape(patch * chans, patch, d)
        wqkv_t = jnp.transpose(w_qkv, (1, 2, 3, 0)).reshape(3 * d, d)
        wo_t = w_out.reshape(d, d)
        w1_t = jnp.transpose(w_fc1, (1, 0))

        def row(v):
            return v.reshape(1, -1)

        hbm = pl.BlockSpec(memory_space=pl.ANY)
        vm = pl.BlockSpec(memory_space=pltpu.VMEM)
        V = pltpu.VMEM
        half = nimg // 2
        out = pl.pallas_call(
            functools.partial(body, cfg),
            out_shape=jax.ShapeDtypeStruct((m, d), BF16),
            in_specs=[hbm, hbm, vm, vm, vm, vm, hbm, vm, hbm, vm, vm, vm, hbm, vm, hbm, vm],
            out_specs=vm,
            scratch_shapes=[
                V(img_t.shape, F32), V((patch * chans, patch, d), BF16), V((chans * 16, 16, d), BF16),
                V((3 * d, d), BF16), V((d, d), BF16), V((ff, d), BF16), V((ff, d), BF16),
                V((half * 2 * chans, 16, width), F32), V((m, chans * 256), BF16),
                V((m, d), BF16), V((m, d), BF16), V((n * tok, d), BF16),
                V((n * tok, d), BF16), V((d, n * tok), F32), V((d, n * tok), F32), V((d, n * tok), F32),
                V((n * tok, d), BF16), V((m, d), BF16), V((m, d), F32), V((m, d), BF16), V((m, d), F32), V((1, d), F32),
                pltpu.SemaphoreType.DMA((7,)), pltpu.SemaphoreType.DMA((nimg,)), pltpu.SemaphoreType.DMA((n,)),
                pltpu.SemaphoreType.DMA((n,)), pltpu.SemaphoreType.DMA((nimg,)),
            ],
            compiler_params=pltpu.CompilerParams(collective_id=0, has_side_effects=True, vmem_limit_bytes=64 * 1024 * 1024 - 128 * 1024),
            name='siglip_layer',
        )(img_t, wp_t, row(b_patch), pos_embed, row(ln1_gain), row(ln1_bias), wqkv_t, b_qkv, wo_t, row(b_out),
          row(ln2_gain), row(ln2_bias), w1_t, row(b_fc1), w_fc2, row(b_fc2))
        return out.reshape(nimg, tok, d)

    in_specs = (P('dp', 'sp', None, None), P(), P(), P('sp', None), P(), P(), P(), P(), P(), P(), P(), P(), P(), P(), P(), P())
    return jax.shard_map(device_step, mesh=mesh, in_specs=in_specs, out_specs=P('dp', 'sp', None), check_vma=False)
```

```python
import functools
import math

import jax
import jax.numpy as jnp
from jax import lax
from jax.experimental import pallas as pl
from jax.experimental.pallas import tpu as pltpu
from jax.sharding import PartitionSpec as P

LN_EPS = 1e-6
F32 = jnp.float32
BF16 = jnp.bfloat16
LOG2E = 1.4426950408889634
NT = (((1,), (1,)), ((), ()))
NN = (((1,), (0,)), ((), ()))


def dot(a, b, dims=NN):
    return lax.dot_general(a, b, dims, preferred_element_type=F32)


def row(v):
    return v[...].reshape(1, v.shape[0])


def norm(z, gain, bias):
    mean = jnp.mean(z, axis=-1, keepdims=True)
    cen = z - mean
    var = jnp.mean(cen * cen, axis=-1, keepdims=True)
    return cen * lax.rsqrt(var + LN_EPS) * gain + bias


def gelu(x):
    inner = math.sqrt(2.0 / math.pi) * (x + 0.044715 * (x * x * x))
    return 0.5 * x * (1.0 + jnp.tanh(inner))


def chunk_transpose(w, chunk):
    rows, lanes = w.shape
    r = lax.broadcasted_iota(jnp.int32, w.shape, 0) % 8
    c = lax.broadcasted_iota(jnp.int32, w.shape, 1) // chunk
    for s in (4, 2, 1):
        up = pltpu.roll(pltpu.roll(w, s * chunk, 1), rows - s, 0)
        down = pltpu.roll(pltpu.roll(w, lanes - s * chunk, 1), s, 0)
        rb, cb = (r & s) != 0, (c & s) != 0
        w = jnp.where(rb == cb, w, jnp.where(cb, up, down))
    return w


def body(cfg, img_hbm, wp_hbm, bp, pos, g1, be1, wqkv_hbm, bqkv, wo_hbm, bo, g2, be2, w1_hbm, b1, w2_hbm, b2, out,
         img, wp_raw, wp, wqkv, wo, w1, w2, zf, xs, x0, y1, yrecv, kall, qt, vt, ot, osend, orecv, res, y2, hid, kbias, sbuf, pbuf,
         wsem, ssem, rsem, ossem, orsem):
    n, nimg, tok, d, heads, hd, ff, patch, chans = cfg
    ntok = n * tok
    per, own = 4, 3
    me = lax.axis_index('sp')
    half = nimg // 2

    def owner(i):
        return per * (i // own) + i % own

    cp_img = [pltpu.make_async_copy(img_hbm.at[pl.ds(half * k, half)], img.at[pl.ds(half * k, half)], wsem.at[k]) for k in range(2)]
    cp_wp = pltpu.make_async_copy(wp_hbm, wp_raw, wsem.at[2])
    cp_wqkv = pltpu.make_async_copy(wqkv_hbm, wqkv, wsem.at[3])
    cp_wo = pltpu.make_async_copy(wo_hbm, wo, wsem.at[4])
    cp_w1 = pltpu.make_async_copy(w1_hbm, w1, wsem.at[5])
    cp_w2 = pltpu.make_async_copy(w2_hbm, w2, wsem.at[6])
    cp_img[0].start()
    cp_img[1].start()
    cp_wp.start()
    barrier = pltpu.get_barrier_semaphore()
    for k in range(1, n):
        pl.semaphore_signal(barrier, inc=1, device_id={'sp': lax.rem(me + k, n)}, device_id_type=pl.DeviceIdType.MESH)

    zf[...] = jnp.zeros_like(zf)
    lrow = lax.broadcasted_iota(jnp.int32, (224, 256), 0)
    lcol = lax.broadcasted_iota(jnp.int32, (224, 256), 1)
    sel = jnp.where((lcol % 16 < patch) & (lrow == patch * (lcol // 16) + lcol % 16), 1.0, 0.0).astype(BF16)
    wp[...] = jnp.zeros_like(wp)

    rows_half = half * tok
    for k in range(2):
        cp_img[k].wait()
        if k == 0:
            cp_wqkv.start()
            cp_wo.start()
            cp_w1.start()
            cp_w2.start()
        for b in range(half):
            for y in range(2):
                for c in range(chans):
                    zf[(b * 2 + y) * chans + c, 0:patch, :] = img[half * k + b, c, patch * y:patch * y + patch, :]
        nz = half * 2 * chans
        u = dot(zf[...].reshape(nz * 16, 224).astype(BF16), sel)
        u = u.reshape(nz, 2, 8, 256)
        for ph in range(2):
            parts = []
            for xh in range(2):
                blk = u[:, ph, :, 128 * xh:128 * xh + 128].reshape(nz * 8, 128)
                parts.append(chunk_transpose(blk, 16).reshape(nz, 1, 8, 128))
            t = jnp.concatenate(parts, axis=1).reshape(half * 2, chans, 16, 128).astype(BF16)
            for c in range(chans):
                xs[pl.ds(rows_half * k, rows_half), 256 * c + 128 * ph:256 * c + 128 * ph + 128] = t[:, c].reshape(rows_half, 128)
        if k == 0:
            cp_wp.wait()
            for c in range(chans):
                for p in range(patch):
                    wp[c * 16 + p, 0:patch, :] = wp_raw[p * chans + c]
        e = dot(xs[pl.ds(rows_half * k, rows_half), :], wp[...].reshape(chans * 256, d))
        base = row(bp) + pos[...].astype(F32)
        e = e + jnp.concatenate([base] * half, axis=0)
        xb = e.astype(BF16)
        x0[pl.ds(rows_half * k, rows_half), :] = xb
        y1[pl.ds(rows_half * k, rows_half), :] = norm(xb.astype(F32), row(g1), row(be1)).astype(BF16)
        if k == 0:
            pl.semaphore_wait(barrier, n - 1)
        for i in range(half * k, half * k + half):
            o = owner(i)

            @pl.when(me != o)
            def _():
                pltpu.make_async_remote_copy(
                    y1.at[pl.ds(tok * i, tok)], yrecv.at[pl.ds(pl.multiple_of(tok * me, tok), tok)],
                    ssem.at[i], rsem.at[me], device_id={'sp': o}, device_id_type=pl.DeviceIdType.MESH).start()

            @pl.when(me == o)
            def _():
                yrecv[pl.ds(pl.multiple_of(tok * me, tok), tok), :] = y1[tok * i:tok * i + tok, :]

    img_idx = own * (me // per) + lax.rem(me, per)

    @pl.when(lax.rem(me, per) < own)
    def _():
        for k in range(1, n):
            s = lax.rem(me + k, n)
            pltpu.make_async_remote_copy(
                y1.at[pl.ds(0, tok)], yrecv.at[pl.ds(pl.multiple_of(tok * s, tok), tok)],
                ssem.at[0], rsem.at[s], device_id={'sp': s}, device_id_type=pl.DeviceIdType.MESH).wait_recv()
        cp_wqkv.wait()
        y = yrecv[...]
        for h in range(heads):
            kbias[0:1, hd * h:hd * h + hd] = bqkv[1, h:h + 1, :]
        for j in range(0, d, 256):
            w = min(256, d - j)
            kall[:, j:j + w] = (dot(y, wqkv[d + j:d + j + w, :], NT) + kbias[0:1, j:j + w]).astype(BF16)
        qbt = jnp.transpose(bqkv[0])
        vbt = jnp.transpose(bqkv[2])
        hh = heads // 2
        for a in range(2):
            qt[pl.ds(hd * hh * a, hd * hh), :] = dot(wqkv[hd * hh * a:hd * hh * a + hd * hh, :], y, NT)
            vt[pl.ds(hd * hh * a, hd * hh), :] = dot(wqkv[2 * d + hd * hh * a:2 * d + hd * hh * a + hd * hh, :], y, NT)
        ntile = 4

        def scores(h):
            win = min(hd * h // 128 * 128, d - 256)
            off = hd * h - win
            pads = [jnp.zeros((k, ntok), F32) if k else None for k in (off, 256 - off - hd)]
            q = qt[hd * h:hd * h + hd, :] + qbt[:, h:h + 1]
            q = jnp.concatenate([z for z in (pads[0], q, pads[1]) if z is not None], axis=0).astype(BF16)
            sbuf[h % ntile] = dot(kall[:, win:win + 256], q)

        def soft(h):
            for b in range(0, ntok, 128):
                s = sbuf[h % ntile, :, b:b + 128]
                m = jnp.max(s, axis=0, keepdims=True)
                p = jnp.exp2((s - m) * (hd ** -0.5 * LOG2E))
                pbuf[h % ntile, :, b:b + 128] = (p * (1.0 / jnp.sum(p, axis=0, keepdims=True))).astype(BF16)

        def mix(h):
            v = (vt[hd * h:hd * h + hd, :] + vbt[:, h:h + 1]).astype(BF16)
            ot[pl.ds(hd * h, hd), :] = dot(v, pbuf[h % ntile])

        for g in range(0, heads + 4, 2):
            for stage, lag in ((scores, 0), (soft, 2), (mix, 4)):
                for h in range(g - lag, g - lag + 2):
                    if 0 <= h < heads:
                        stage(h)
        eye = jnp.where(lax.broadcasted_iota(jnp.int32, (ntok, ntok), 0) == lax.broadcasted_iota(jnp.int32, (ntok, ntok), 1),
                        1.0, 0.0).astype(BF16)
        for j in range(0, d, 256):
            w = min(256, d - j)
            osend[:, j:j + w] = dot(eye, ot[j:j + w, :].astype(BF16), NT).astype(BF16)
        for k in (4, 5, 3, 2, 6, 7, 1):
            s = lax.rem(me + k, n)
            pltpu.make_async_remote_copy(
                osend.at[pl.ds(pl.multiple_of(tok * s, tok), tok)], orecv.at[pl.ds(pl.multiple_of(tok * img_idx, tok), tok)],
                ossem.at[s], orsem.at[img_idx], device_id={'sp': s}, device_id_type=pl.DeviceIdType.MESH).start()
        orecv[pl.ds(pl.multiple_of(tok * img_idx, tok), tok), :] = osend[pl.ds(pl.multiple_of(tok * me, tok), tok), :]

    @pl.when(lax.rem(me, per) >= own)
    def _():
        cp_wqkv.wait()

    for i in range(nimg):
        o = owner(i)

        @pl.when(me != o)
        def _():
            pltpu.make_async_remote_copy(
                osend.at[pl.ds(0, tok)], orecv.at[pl.ds(tok * i, tok)],
                ossem.at[0], orsem.at[i], device_id={'sp': o}, device_id_type=pl.DeviceIdType.MESH).wait_recv()

    cp_wo.wait()
    r = x0[...].astype(F32) + dot(orecv[...], wo[...]) + row(bo)
    res[...] = r
    y2[...] = norm(r, row(g2), row(be2)).astype(BF16)
    cp_w1.wait()
    cp_w2.wait()
    step = 512
    for c in range(0, ff, step):
        w = min(step, ff - c)
        h = dot(y2[...], w1[c:c + w, :], NT) + b1[pl.ds(c, w)].reshape(1, w)
        hid[:, c:c + w] = gelu(h).astype(BF16)
    for j in range(0, d, 256):
        w = min(256, d - j)
        acc = res[:, j:j + w] + dot(hid[...], w2[:, j:j + w])
        out[:, j:j + w] = (acc + b2[pl.ds(j, w)].reshape(1, w)).astype(BF16)

    for i in range(nimg):
        o = owner(i)

        @pl.when(me != o)
        def _():
            pltpu.make_async_remote_copy(
                y1.at[pl.ds(tok * i, tok)], yrecv.at[pl.ds(0, tok)],
                ssem.at[i], rsem.at[0], device_id={'sp': o}, device_id_type=pl.DeviceIdType.MESH).wait_send()

    @pl.when(lax.rem(me, per) < own)
    def _():
        for k in range(1, n):
            s = lax.rem(me + k, n)
            pltpu.make_async_remote_copy(
                osend.at[pl.ds(0, tok)], orecv.at[pl.ds(0, tok)],
                ossem.at[s], orsem.at[0], device_id={'sp': s}, device_id_type=pl.DeviceIdType.MESH).wait_send()


def solution(mesh):
    n = mesh.shape['sp']

    def device_step(images, w_patch, b_patch, pos_embed, ln1_gain, ln1_bias, w_qkv, b_qkv, w_out, b_out, ln2_gain, ln2_bias, w_fc1, b_fc1, w_fc2, b_fc2):
        nimg, rows, width, chans = images.shape
        tok, d = pos_embed.shape
        patch = w_patch.shape[0]
        _, _, heads, hd = w_qkv.shape
        ff = w_fc1.shape[1]
        m = nimg * tok
        cfg = (n, nimg, tok, d, heads, hd, ff, patch, chans)
        img_t = jnp.transpose(images, (0, 3, 1, 2))
        wp_t = jnp.transpose(w_patch, (0, 2, 1, 3)).reshape(patch * chans, patch, d)
        wqkv_t = jnp.transpose(w_qkv, (1, 2, 3, 0)).reshape(3 * d, d)
        wo_t = w_out.reshape(d, d)
        w1_t = jnp.transpose(w_fc1, (1, 0))

        hbm = pl.BlockSpec(memory_space=pl.ANY)
        vm = pl.BlockSpec(memory_space=pltpu.VMEM)
        V = pltpu.VMEM
        half = nimg // 2
        out = pl.pallas_call(
            functools.partial(body, cfg),
            out_shape=jax.ShapeDtypeStruct((m, d), BF16),
            in_specs=[hbm, hbm, vm, vm, vm, vm, hbm, vm, hbm, vm, vm, vm, hbm, vm, hbm, vm],
            out_specs=vm,
            scratch_shapes=[
                V(img_t.shape, F32), V((patch * chans, patch, d), BF16), V((chans * 16, 16, d), BF16),
                V((3 * d, d), BF16), V((d, d), BF16), V((ff, d), BF16), V((ff, d), BF16),
                V((half * 2 * chans, 16, width), F32), V((m, chans * 256), BF16),
                V((m, d), BF16), V((m, d), BF16), V((n * tok, d), BF16),
                V((n * tok, d), BF16), V((d, n * tok), F32), V((d, n * tok), F32), V((d, n * tok), F32),
                V((n * tok, d), BF16), V((m, d), BF16), V((m, d), F32), V((m, d), BF16), V((m, ff), BF16), V((1, d), F32),
                V((4, n * tok, n * tok), F32), V((4, n * tok, n * tok), BF16),
                pltpu.SemaphoreType.DMA((7,)), pltpu.SemaphoreType.DMA((nimg,)), pltpu.SemaphoreType.DMA((n,)),
                pltpu.SemaphoreType.DMA((n,)), pltpu.SemaphoreType.DMA((nimg,)),
            ],
            compiler_params=pltpu.CompilerParams(collective_id=0, has_side_effects=True, vmem_limit_bytes=64 * 1024 * 1024 - 128 * 1024),
            name='siglip_layer',
        )(img_t, wp_t, b_patch, pos_embed, ln1_gain, ln1_bias, wqkv_t, b_qkv, wo_t, b_out,
          ln2_gain, ln2_bias, w1_t, b_fc1, w_fc2, b_fc2)
        return out.reshape(nimg, tok, d)

    in_specs = (P('dp', 'sp', None, None), P(), P(), P('sp', None), P(), P(), P(), P(), P(), P(), P(), P(), P(), P(), P(), P())
    return jax.shard_map(device_step, mesh=mesh, in_specs=in_specs, out_specs=P('dp', 'sp', None), check_vma=False)
```

```python
import functools
import math

import jax
import jax.numpy as jnp
from jax import lax
from jax.experimental import pallas as pl
from jax.experimental.pallas import tpu as pltpu
from jax.sharding import PartitionSpec as P

LN_EPS = 1e-6
LOG2E = 1.4426950408889634
F32 = jnp.float32
BF16 = jnp.bfloat16
NT = (((1,), (1,)), ((), ()))
NN = (((1,), (0,)), ((), ()))
MESH = pl.DeviceIdType.MESH


def dot(a, b, dims=NN):
    return lax.dot_general(a, b, dims, preferred_element_type=F32)


def row(v):
    return v[...].reshape(1, v.shape[0])


def norm(z, gain, bias):
    mean = jnp.mean(z, axis=-1, keepdims=True)
    cen = z - mean
    var = jnp.mean(cen * cen, axis=-1, keepdims=True)
    return cen * lax.rsqrt(var + LN_EPS) * gain + bias


def gelu(x):
    inner = math.sqrt(2.0 / math.pi) * (x + 0.044715 * (x * x * x))
    return 0.5 * x * (1.0 + jnp.tanh(inner))


def chunk_transpose(w, chunk):
    rows, lanes = w.shape
    r = lax.broadcasted_iota(jnp.int32, w.shape, 0) % 8
    c = lax.broadcasted_iota(jnp.int32, w.shape, 1) // chunk
    for s in (4, 2, 1):
        up = pltpu.roll(pltpu.roll(w, s * chunk, 1), rows - s, 0)
        down = pltpu.roll(pltpu.roll(w, lanes - s * chunk, 1), s, 0)
        rb, cb = (r & s) != 0, (c & s) != 0
        w = jnp.where(rb == cb, w, jnp.where(cb, up, down))
    return w


def pack_heads(heads):
    out = []
    shape = (heads[0].shape[0], 128)
    lane = lax.broadcasted_iota(jnp.int32, shape, 1)
    upper, odd = lane >= 64, (lane // 32) % 2 == 1
    for t in range(0, heads[0].shape[1], 128):
        a = [x[:, t:t + 128] for x in heads]
        b = [None] * 4
        for j in (0, 1):
            b[j] = jnp.where(upper, pltpu.roll(a[j + 2], 64, 1), a[j])
            b[j + 2] = jnp.where(upper, a[j + 2], pltpu.roll(a[j], 64, 1))
        for j in (0, 2):
            out.append(jnp.where(odd, pltpu.roll(b[j + 1], 32, 1), b[j]))
            out.append(jnp.where(odd, b[j + 1], pltpu.roll(b[j], 96, 1)))
    return out


def body(cfg, *refs):
    n, nimg, tok, d, heads, hd, ff, patch, chans = cfg
    (img_hbm, wp_hbm, bp_h, pos_h, g1_h, be1_h, wqkv_hbm, bqkv_h, wo_hbm, bo_h, g2_h, be2_h, w1_hbm, b1_h, w2_hbm, b2_h, out,
     img, wp_raw, wp, wq, wo, w1, w2, bp, pos, g1, be1, bqkv, bo, g2, be2, b1, b2,
     zf, xs, x0, y1, yrecv, qkv, sbuf, pbuf, bsc, bcol, osend, orecv, og, res, y2, hid,
     isem, wsem, qsem, vsem, ssem, rsem, fsem, frsem, ossem, orsem) = refs
    ntok = n * tok
    gh, ng = 4, 3
    gw = gh * hd
    me = lax.axis_index('sp')
    chip, core = me // 2, lax.rem(me, 2)
    pair, side = chip // 2, lax.rem(chip, 2)
    img_full, img_split = 3 * pair + 2 * side, 3 * pair + 1

    def image_of(e):
        return 3 * (e // 4) + (e % 4 if e % 4 < 3 else 1)

    def source_of(i, hg):
        if i % 3 == 1:
            return 2 * (2 * (i // 3) + hg // 2) + 1
        return 2 * (2 * (i // 3) + (i % 3) // 2) + (1 if hg == 0 else 0)

    def send_y(i, src_row, e, slot):
        return pltpu.make_async_remote_copy(
            y1.at[pl.ds(src_row, tok)], yrecv.at[0, pl.ds(pl.multiple_of(tok * slot, tok), tok)],
            ssem.at[i], rsem.at[slot], device_id={'sp': e}, device_id_type=MESH)

    def forward(s, dst):
        rows = pl.ds(pl.multiple_of(tok * s, tok), tok)
        return pltpu.make_async_remote_copy(
            yrecv.at[0, rows], yrecv.at[1, rows], fsem.at[s], frsem.at[s], device_id={'sp': dst}, device_id_type=MESH)

    def send_o(g, s, hg, i):
        return pltpu.make_async_remote_copy(
            osend.at[g, s], orecv.at[hg, i], ossem.at[g, s], orsem.at[hg, i], device_id={'sp': s}, device_id_type=MESH)

    def head_group(g):
        if g < 2:
            return (1 - core) * (g + 1) + core * (2 * side + g)
        return (1 - core) * 3

    batches = ([i for i in range(nimg) if i % 3 == 1], [i for i in range(nimg) if i % 3 != 1])
    cp_img = [pltpu.make_async_copy(img_hbm.at[i], img.at[i], isem.at[i]) for i in range(nimg)]
    cp_wp = pltpu.make_async_copy(wp_hbm, wp_raw, wsem.at[0])
    cp_wo = pltpu.make_async_copy(wo_hbm, wo, wsem.at[1])
    cp_w1 = pltpu.make_async_copy(w1_hbm, w1, wsem.at[2])
    cp_w2 = pltpu.make_async_copy(w2_hbm, w2, wsem.at[3])
    cp_q = [pltpu.make_async_copy(
        wqkv_hbm.at[pl.ds(pl.multiple_of(d * t + gw * head_group(g), 32), gw)], wq.at[g, pl.ds(gw * t, gw)], qsem.at[g, t])
        for g in range(ng) for t in range(3)]
    cp_v = [pltpu.make_async_copy(a, b, vsem.at[k]) for k, (a, b) in enumerate(
        ((bp_h, bp), (pos_h, pos), (g1_h, g1), (be1_h, be1), (bqkv_h, bqkv), (bo_h, bo), (g2_h, g2), (be2_h, be2), (b1_h, b1), (b2_h, b2)))]
    for i in batches[0] + batches[1]:
        cp_img[i].start()
    cp_wp.start()
    for c in cp_v:
        c.start()
    barrier = pltpu.get_barrier_semaphore()
    for k in range(1, n):
        pl.semaphore_signal(barrier, inc=1, device_id={'sp': lax.rem(me + k, n)}, device_id_type=MESH)

    zf[...] = jnp.zeros_like(zf)
    lrow = lax.broadcasted_iota(jnp.int32, (224, 256), 0)
    lcol = lax.broadcasted_iota(jnp.int32, (224, 256), 1)
    sel = jnp.where((lcol % 16 < patch) & (lrow == patch * (lcol // 16) + lcol % 16), 1.0, 0.0).astype(BF16)
    wp[...] = jnp.zeros_like(wp)

    for bi, batch in enumerate(batches):
        nb = len(batch)
        for i in batch:
            cp_img[i].wait()
        if bi == len(batches) - 1:
            for c in cp_q:
                c.start()
            cp_wo.start()
            cp_w1.start()
            cp_w2.start()
        for b, i in enumerate(batch):
            for y in range(2):
                for c in range(chans):
                    zf[(b * 2 + y) * chans + c, 0:patch, :] = img[i, c, patch * y:patch * y + patch, :]
        nz = nb * 2 * chans
        u = dot(zf[0:nz].reshape(nz * 16, 224).astype(BF16), sel)
        u = u.reshape(nz, 2, 8, 256)
        for ph in range(2):
            parts = []
            for xh in range(2):
                blk = u[:, ph, :, 128 * xh:128 * xh + 128].reshape(nz * 8, 128)
                parts.append(chunk_transpose(blk, 16).reshape(nz, 1, 8, 128))
            t = jnp.concatenate(parts, axis=1).reshape(nb * 2, chans, 16, 128).astype(BF16)
            for c in range(chans):
                xs[0:nb * tok, 256 * c + 128 * ph:256 * c + 128 * ph + 128] = t[:, c].reshape(nb * tok, 128)
        if bi == 0:
            cp_wp.wait()
            for c in cp_v:
                c.wait()
            for c in range(chans):
                for p in range(patch):
                    wp[c * 16 + p, 0:patch, :] = wp_raw[p * chans + c]
        e = dot(xs[0:nb * tok, :], wp[...].reshape(chans * 256, d))
        base = row(bp) + pos[...].astype(F32)
        xb = (e + jnp.concatenate([base] * nb, axis=0)).astype(BF16)
        yb = norm(xb.astype(F32), row(g1), row(be1)).astype(BF16)
        for b, i in enumerate(batch):
            x0[tok * i:tok * i + tok, :] = xb[tok * b:tok * b + tok, :]
            y1[tok * i:tok * i + tok, :] = yb[tok * b:tok * b + tok, :]
        if bi == 0:
            pl.semaphore_wait(barrier, n - 1)
        for e in range(n):
            i = image_of(e)
            if i not in batch:
                continue

            @pl.when(me != e)
            def _():
                send_y(e, tok * i, e, me).start()

            @pl.when(me == e)
            def _():
                yrecv[0, pl.ds(pl.multiple_of(tok * me, tok), tok), :] = y1[tok * i:tok * i + tok, :]

    for t in range(3):
        for hg in range(heads // gh):
            bsc[t, hg, 0:gh, :] = bqkv[t, gh * hg:gh * hg + gh, :]
    for g in range(ng):
        for t in range(3):
            bcol[g, t] = jnp.transpose(bsc[t, head_group(g)])
    res[...] = x0[...].astype(F32) + row(bo)

    def project(g, slot, parts):
        for t in parts:
            qkv[g % 2, gw * t:gw * t + gw, :] = dot(wq[g, gw * t:gw * t + gw, :], yrecv[slot], NT)

    def head(g, t, j):
        return qkv[g % 2, gw * t + hd * j:gw * t + hd * j + hd, :] + bcol[g, t, :, j:j + 1]

    def scores(g, j):
        sbuf[j] = dot(jnp.transpose(head(g, 1, j)).astype(BF16), head(g, 0, j).astype(BF16))

    def soft(j):
        for b in range(0, ntok, 128):
            s = sbuf[j, :, b:b + 128]
            p = jnp.exp2((s - jnp.max(s, axis=0, keepdims=True)) * (hd ** -0.5 * LOG2E))
            pbuf[j, :, b:b + 128] = (p * (1.0 / jnp.sum(p, axis=0, keepdims=True))).astype(BF16)

    def mix(g, j):
        return dot(head(g, 2, j).astype(BF16), pbuf[j])

    def run_groups(gs, slot, i):
        for t in range(3):
            cp_q[3 * gs[0] + t].wait()
        project(gs[0], slot, range(3))
        for g in gs:
            if g + 1 in gs:
                for t in range(3):
                    cp_q[3 * (g + 1) + t].wait()
            for j in range(gh):
                scores(g, j)
            outs = []
            for j in range(gh):
                if g + 1 in gs and j < 3:
                    project(g + 1, slot, (j,))
                soft(j)
                if j:
                    outs.append(mix(g, j - 1))
            outs.append(mix(g, gh - 1))
            for e, o in enumerate(pack_heads(outs)):
                osend[g, e] = o.astype(BF16)
            hg = head_group(g)
            for k in (4, 5, 3, 2, 6, 7, 1):
                send_o(g, lax.rem(me + k, n), hg, i).start()
            orecv[hg, i] = osend[g, me]


    @pl.when(core == 0)
    def _():
        for k in (0, 1, 2, 3, 6, 7, 4, 5):
            s = lax.rem(me + k, n)
            if k:
                send_y(0, 0, s, s).wait_recv()
            forward(s, me + 1).start()
        run_groups((0, 1, 2), 0, img_full)

    @pl.when(core == 1)
    def _():
        for k in range(1, n):
            s = lax.rem(me + k, n)
            send_y(0, 0, s, s).wait_recv()
        run_groups((0, 1), 0, img_split)
        for s in range(n):
            forward(s, me - 1).wait_recv()
        run_groups((2,), 1, img_full)

    cp_wo.wait()
    for hg in (1, 0, 2, 3):
        for i in range(nimg):
            src = source_of(i, hg)

            @pl.when(me != src)
            def _():
                send_o(0, src, hg, i).wait_recv()
        for i in range(nimg):
            t = jnp.transpose(orecv[hg, i].astype(F32))
            for j in range(gh):
                og[tok * i:tok * i + tok, hd * j:hd * j + hd] = t[tok * j:tok * j + tok, :]
        res[...] += dot(og[...].astype(BF16), wo[gw * hg:gw * hg + gw, :])

    y2[...] = norm(res[...], row(g2), row(be2)).astype(BF16)
    cp_w1.wait()
    cp_w2.wait()
    step = 512
    for c in range(0, ff, step):
        w = min(step, ff - c)
        h = dot(y2[...], w1[c:c + w, :], NT) + b1[pl.ds(c, w)].reshape(1, w)
        hid[:, c:c + w] = gelu(h).astype(BF16)
    for j in range(0, d, 256):
        w = min(256, d - j)
        acc = res[:, j:j + w] + dot(hid[...], w2[:, j:j + w])
        out[:, j:j + w] = (acc + b2[pl.ds(j, w)].reshape(1, w)).astype(BF16)
    for e in range(n):
        @pl.when(me != e)
        def _():
            send_y(e, 0, e, 0).wait_send()

    @pl.when(core == 0)
    def _():
        for s in range(n):
            forward(s, me + 1).wait_send()

    for g in range(ng):
        for k in range(1, n):
            s = lax.rem(me + k, n)
            send_o(g, s, 0, 0).wait_send()


def solution(mesh):
    n = mesh.shape['sp']

    def device_step(images, w_patch, b_patch, pos_embed, ln1_gain, ln1_bias, w_qkv, b_qkv, w_out, b_out, ln2_gain, ln2_bias, w_fc1, b_fc1, w_fc2, b_fc2):
        nimg, rows, width, chans = images.shape
        tok, d = pos_embed.shape
        patch = w_patch.shape[0]
        _, _, heads, hd = w_qkv.shape
        ff = w_fc1.shape[1]
        m = nimg * tok
        ntok = n * tok
        cfg = (n, nimg, tok, d, heads, hd, ff, patch, chans)
        img_t = jnp.transpose(images, (0, 3, 1, 2))
        wp_t = jnp.transpose(w_patch, (0, 2, 1, 3)).reshape(patch * chans, patch, d)
        wqkv_t = jnp.transpose(w_qkv, (1, 2, 3, 0)).reshape(3 * d, d)
        wo_t = w_out.reshape(d, d)
        w1_t = jnp.transpose(w_fc1, (1, 0))

        hbm = pl.BlockSpec(memory_space=pl.ANY)
        V, S = pltpu.VMEM, pltpu.SemaphoreType.DMA
        out = pl.pallas_call(
            functools.partial(body, cfg),
            out_shape=jax.ShapeDtypeStruct((m, d), BF16),
            in_specs=[hbm] * 16,
            out_specs=pl.BlockSpec(memory_space=pltpu.VMEM),
            scratch_shapes=[
                V(img_t.shape, F32), V((patch * chans, patch, d), BF16), V((chans * 16, 16, d), BF16),
                V((3, 12 * hd, d), BF16), V((d, d), BF16), V((ff, d), BF16), V((ff, d), BF16),
                V((d,), F32), V((tok, d), BF16), V((d,), F32), V((d,), F32), V((3, heads, hd), F32), V((d,), F32), V((d,), F32),
                V((d,), F32), V((ff,), F32), V((d,), F32),
                V((8 * chans, 16, width), F32), V((4 * tok, chans * 256), BF16),
                V((m, d), BF16), V((m, d), BF16), V((2, ntok, d), BF16),
                V((2, 12 * hd, ntok), F32), V((4, ntok, ntok), F32), V((4, ntok, ntok), BF16),
                V((3, 4, 8, hd), F32), V((3, 3, hd, 8), F32),
                V((3, n, hd, 128), BF16), V((4, nimg, hd, 128), BF16), V((m, 4 * hd), F32), V((m, d), F32), V((m, d), BF16), V((m, ff), BF16),
                S((nimg,)), S((4,)), S((3, 3)), S((10,)), S((n,)), S((n,)), S((n,)), S((n,)), S((3, n)), S((4, nimg)),
            ],
            compiler_params=pltpu.CompilerParams(collective_id=0, has_side_effects=True, vmem_limit_bytes=64 * 1024 * 1024 - 128 * 1024),
            name='siglip_layer',
        )(img_t, wp_t, b_patch, pos_embed, ln1_gain, ln1_bias, wqkv_t, b_qkv, wo_t, b_out,
          ln2_gain, ln2_bias, w1_t, b_fc1, w_fc2, b_fc2)
        return out.reshape(nimg, tok, d)

    in_specs = (P('dp', 'sp', None, None), P(), P(), P('sp', None), P(), P(), P(), P(), P(), P(), P(), P(), P(), P(), P(), P())
    return jax.shard_map(device_step, mesh=mesh, in_specs=in_specs, out_specs=P('dp', 'sp', None), check_vma=False)
```

```python
import functools
import math

import jax
import jax.numpy as jnp
from jax import lax
from jax.experimental import pallas as pl
from jax.experimental.pallas import tpu as pltpu
from jax.sharding import PartitionSpec as P

LN_EPS = 1e-6
LOG2E = 1.4426950408889634
F32 = jnp.float32
BF16 = jnp.bfloat16
NT = (((1,), (1,)), ((), ()))
NN = (((1,), (0,)), ((), ()))
MESH = pl.DeviceIdType.MESH


def dot(a, b, dims=NN):
    return lax.dot_general(a, b, dims, preferred_element_type=F32)


def row(v):
    return v[...].reshape(1, v.shape[0])


def norm(z, gain, bias):
    mean = jnp.mean(z, axis=-1, keepdims=True)
    cen = z - mean
    var = jnp.mean(cen * cen, axis=-1, keepdims=True)
    return cen * lax.rsqrt(var + LN_EPS) * gain + bias


def gelu(x):
    inner = math.sqrt(2.0 / math.pi) * (x + 0.044715 * (x * x * x))
    return 0.5 * x * (1.0 + jnp.tanh(inner))


def chunk_transpose(w, chunk):
    rows, lanes = w.shape
    r = lax.broadcasted_iota(jnp.int32, w.shape, 0) % 8
    c = lax.broadcasted_iota(jnp.int32, w.shape, 1) // chunk
    for s in (4, 2, 1):
        up = pltpu.roll(pltpu.roll(w, s * chunk, 1), rows - s, 0)
        down = pltpu.roll(pltpu.roll(w, lanes - s * chunk, 1), s, 0)
        rb, cb = (r & s) != 0, (c & s) != 0
        w = jnp.where(rb == cb, w, jnp.where(cb, up, down))
    return w


def body(cfg, *refs):
    n, nimg, tok, d, heads, hd, ff, patch, chans = cfg
    (img_hbm, wp_hbm, bp_h, pos_h, g1_h, be1_h, wqkv_hbm, bqkv_h, wo_hbm, bo_h, g2_h, be2_h, w1_hbm, b1_h, w2_hbm, b2_h, out_hbm, out,
     img, wp_raw, wp, wq, wo, w1s, w1t, w2, bp, pos, g1, be1, bqkv, bo, g2, be2, b1, b2,
     zf, xs, x0, y1, yrecv, qkv, sbuf, pbuf, bsc, bcol, osend, orecv, res, y2, hid,
     outsem, isem, wsem, psem, qsem, csem, vsem, ssem, rsem, fsem, frsem, ossem, orsem) = refs
    ntok = n * tok
    gh, ng = 4, 4
    step, slots = w1s.shape[1], w1s.shape[0]
    gw = gh * hd
    me = lax.axis_index('sp')
    chip, core = me // 2, lax.rem(me, 2)
    pair, side = chip // 2, lax.rem(chip, 2)
    nxt = lax.rem(me + 1, n)
    pos_split, pos_full = pair, 2 + chip
    order = [i for i in range(nimg) if i % 3 == 1] + [i for i in range(nimg) if i % 3 != 1]

    def source_of(p, hg):
        return 2 * (2 * p + hg // 2) + 1 if p < 2 else 2 * (p - 2) + hg // 2

    def send_y(i, src_row, e, slot):
        return pltpu.make_async_remote_copy(
            y1.at[pl.ds(src_row, tok)], yrecv.at[0, pl.ds(pl.multiple_of(tok * slot, tok), tok)],
            ssem.at[i], rsem.at[slot], device_id={'sp': e}, device_id_type=MESH)

    def wait_sent(bi):
        for here in range(2):
            rows = pl.ds(0, tok * (n // 2 - (here != bi)))

            @pl.when(core == here)
            def _():
                pltpu.make_async_remote_copy(
                    yrecv.at[0, rows], yrecv.at[1, rows], ssem.at[bi], rsem.at[0], device_id={'sp': nxt}, device_id_type=MESH).wait_send()

    def forward(s, dst):
        rows = pl.ds(pl.multiple_of(tok * s, tok), tok)
        return pltpu.make_async_remote_copy(
            yrecv.at[0, rows], yrecv.at[1, rows], fsem.at[0], frsem.at[0], device_id={'sp': dst}, device_id_type=MESH)

    def forward_all(dst):
        return pltpu.make_async_remote_copy(
            yrecv.at[0], yrecv.at[1], fsem.at[0], frsem.at[0], device_id={'sp': dst}, device_id_type=MESH)

    def wave_of(g):
        return 1 - core if g < 2 else 1

    def send_o(g, s, hg, i):
        return pltpu.make_async_remote_copy(
            osend.at[g, pl.ds(pl.multiple_of(tok * s, tok), tok)], orecv.at[hg, pl.ds(pl.multiple_of(tok * i, tok), tok)],
            ossem.at[g], orsem.at[hg, wave_of(g)], device_id={'sp': s}, device_id_type=MESH)

    def head_group(g):
        return (1 - core) * g + core * (2 * side + g) if g < 2 else g

    def w1_copy(c, slot, size):
        start = c * step if isinstance(c, int) else pl.multiple_of(c * step, step)
        return pltpu.make_async_copy(w1_hbm.at[pl.ds(start, size)], w1s.at[slot, pl.ds(0, size)], csem.at[slot])

    batches = (order[:2], order[2:])
    bounds = (0, 2, nimg)
    cp_img = [pltpu.make_async_copy(img_hbm.at[i], img.at[i], isem.at[0 if i in order[:2] else 1]) for i in range(nimg)]
    cp_wp = [pltpu.make_async_copy(wp_hbm, wp_raw, psem.at[0])]
    cp_wo = pltpu.make_async_copy(wo_hbm, wo, wsem.at[0])
    cp_w2 = pltpu.make_async_copy(w2_hbm, w2, wsem.at[1])
    cp_q = [pltpu.make_async_copy(
        wqkv_hbm.at[pl.ds(pl.multiple_of(d * t + gw * head_group(g), 32), gw)], wq.at[g, pl.ds(gw * t, gw)], qsem.at[g])
        for g in range(ng) for t in range(3)]
    cp_v = [pltpu.make_async_copy(a, b, vsem.at[k]) for k, (a, b) in enumerate(
        ((bp_h, bp), (pos_h, pos), (g1_h, g1), (be1_h, be1), (bqkv_h, bqkv), (bo_h, bo), (g2_h, g2), (be2_h, be2), (b1_h, b1), (b2_h, b2)))]
    for c in cp_wp + [cp_img[i] for i in batches[0]] + cp_v[:4] + [cp_img[i] for i in batches[1]] + cp_v[4:]:
        c.start()
    wp[...] = jnp.zeros_like(wp)
    barrier = pltpu.get_barrier_semaphore()
    for k in range(1, n):
        pl.semaphore_signal(barrier, inc=1, device_id={'sp': lax.rem(me + k, n)}, device_id_type=MESH)

    zf[...] = jnp.zeros_like(zf)
    lrow = lax.broadcasted_iota(jnp.int32, (224, 256), 0)
    lcol = lax.broadcasted_iota(jnp.int32, (224, 256), 1)
    sel = jnp.where((lcol % 16 < patch) & (lrow == patch * (lcol // 16) + lcol % 16), 1.0, 0.0).astype(BF16)

    full, early = ff // step, 3
    rest = ff - full * step

    def turn(c, size, slot):
        w1t[:, pl.ds(c * step if isinstance(c, int) else pl.multiple_of(c * step, step), size)] = jnp.transpose(w1s[slot, 0:size])

    def turn_step(c, carry):
        slot = lax.rem(c, slots)
        w1_copy(c, slot, step).wait()
        turn(c, step, slot)

        @pl.when(c + slots < full)
        def _():
            w1_copy(c + slots, slot, step).start()

        @pl.when(c + slots == full)
        def _():
            w1_copy(full, slot, rest).start()

        return carry

    for bi, batch in enumerate(batches):
        nb = len(batch)
        pltpu.make_async_copy(img_hbm.at[pl.ds(0, nb)], img.at[pl.ds(0, nb)], isem.at[bi]).wait()
        if bi == len(batches) - 1:
            for c in cp_q[:6]:
                c.start()
        for b, i in enumerate(batch):
            for y in range(2):
                for c in range(chans):
                    zf[(b * 2 + y) * chans + c, 0:patch, :] = img[i, c, patch * y:patch * y + patch, :]
        nz = nb * 2 * chans
        u = dot(zf[0:nz].reshape(nz * 16, 224).astype(BF16), sel)
        u = u.reshape(nz, 2, 8, 256)
        for ph in range(2):
            parts = []
            for xh in range(2):
                blk = u[:, ph, :, 128 * xh:128 * xh + 128].reshape(nz * 8, 128)
                parts.append(chunk_transpose(blk, 16).reshape(nz, 1, 8, 128))
            t = jnp.concatenate(parts, axis=1).reshape(nb * 2, chans, 16, 128).astype(BF16)
            for c in range(chans):
                xs[0:nb * tok, 256 * c + 128 * ph:256 * c + 128 * ph + 128] = t[:, c].reshape(nb * tok, 128)
        if bi == 0:
            for c in cp_wp + cp_v[:4]:
                c.wait()
            for c in range(slots):
                w1_copy(c, c, step).start()
            for c in range(chans):
                for p in range(patch):
                    wp[c, p, 0:patch, :] = wp_raw[p, c]
        e = dot(xs[0:nb * tok, :], wp[...].reshape(chans * 256, d))
        base = row(bp) + pos[...].astype(F32)
        xb = (e + jnp.concatenate([base] * nb, axis=0)).astype(BF16)
        yb = norm(xb.astype(F32), row(g1), row(be1)).astype(BF16)
        x0[tok * bounds[bi]:tok * bounds[bi + 1], :] = xb
        y1[tok * bounds[bi]:tok * bounds[bi + 1], :] = yb
        if bi == 0:
            pl.semaphore_wait(barrier, n - 1)
        if bi == 1:
            lax.fori_loop(0, early, turn_step, 0)
            wait_sent(0)
        for k in (2, 1, 3, 0):
            c = lax.rem(chip + k, n // 2)
            if bi == 0:
                e, p = 2 * c + 1, c // 2
            else:
                e, p = 2 * c, 2 + c
            src = pl.multiple_of(tok * p, tok)

            @pl.when(me != e)
            def _():
                send_y(bi, src, e, me).start()

            @pl.when(me == e)
            def _():
                yrecv[0, pl.ds(pl.multiple_of(tok * me, tok), tok), :] = y1[pl.ds(src, tok), :]

    for c in cp_v[4:]:
        c.wait()
    for t in range(3):
        for hg in range(heads // gh):
            bsc[t, hg, 0:gh, :] = bqkv[t, gh * hg:gh * hg + gh, :]
    for g in range(ng):
        for t in range(3):
            bcol[g, t] = jnp.transpose(bsc[t, head_group(g)])
    res[...] = x0[...].astype(F32) + row(bo)
    lax.fori_loop(early, full, turn_step, 0)

    @pl.when(core == 1)
    def _():
        for c in cp_q[6:]:
            c.start()

    cp_wo.start()
    cp_w2.start()
    w1_copy(full, full % slots, rest).wait()
    turn(full, rest, full % slots)

    def project(g, slot, parts):
        for t in parts:
            qkv[g % 2, gw * t:gw * t + gw, :] = dot(wq[g, gw * t:gw * t + gw, :], yrecv[slot], NT)

    def head(g, t, j):
        return qkv[g % 2, gw * t + hd * j:gw * t + hd * j + hd, :] + bcol[g, t, :, j:j + 1]

    def scores(g, j):
        sbuf[j] = dot(jnp.transpose(head(g, 1, j)).astype(BF16), head(g, 0, j).astype(BF16))

    def soft(j):
        for b in range(0, ntok, 128):
            s = sbuf[j, :, b:b + 128]
            p = jnp.exp2((s - jnp.max(s, axis=0, keepdims=True)) * (hd ** -0.5 * LOG2E))
            pbuf[j, :, b:b + 128] = (p * (1.0 / jnp.sum(p, axis=0, keepdims=True))).astype(BF16)

    def mix(g, j):
        return dot(head(g, 2, j).astype(BF16), pbuf[j])

    def wait_q(g):
        pltpu.make_async_copy(wqkv_hbm.at[pl.ds(0, 3 * gw)], wq.at[g], qsem.at[g]).wait()

    def run_groups(gs, slot, i):
        wait_q(gs[0])
        project(gs[0], slot, range(3))
        for g in gs:
            if g + 1 in gs:
                wait_q(g + 1)
            for j in range(gh):
                scores(g, j)
            outs = []
            for j in range(gh):
                if g + 1 in gs and j < 3:
                    project(g + 1, slot, (j,))
                soft(j)
                if j:
                    outs.append(mix(g, j - 1))
            outs.append(mix(g, gh - 1))
            osend[g] = jnp.transpose(jnp.concatenate(outs, axis=0)).astype(BF16)
            hg = head_group(g)
            for k in (4, 5, 3, 2, 6, 7, 1):
                send_o(g, lax.rem(me + k, n), hg, i).start()
            orecv[hg, pl.ds(pl.multiple_of(tok * i, tok), tok), :] = osend[g, pl.ds(pl.multiple_of(tok * me, tok), tok), :]


    @pl.when(core == 0)
    def _():
        for k in (0, 1, 2, 3, 6, 7, 4, 5):
            s = lax.rem(me + k, n)
            if k:
                send_y(0, 0, s, s).wait_recv()
            forward(s, me + 1).start()
        run_groups((0, 1), 0, pos_full)

    @pl.when(core == 1)
    def _():
        for k in range(1, n):
            s = lax.rem(me + k, n)
            send_y(0, 0, s, s).wait_recv()
        run_groups((0, 1), 0, pos_split)
        forward_all(me - 1).wait_recv()
        run_groups((2, 3), 1, pos_full)

    cp_wo.wait()
    for w in range(2):
        lo, hi = bounds[w], bounds[w + 1]
        rows = slice(tok * lo, tok * hi)
        for hg in (0, 2, 1, 3):
            mine = sum(jnp.where(me == source_of(p, hg), 1, 0) for p in range(lo, hi))
            for k in range(2):
                got = pl.ds(0, tok * (hi - lo - k))

                @pl.when(mine == k)
                def _():
                    pltpu.make_async_remote_copy(
                        osend.at[0, got], orecv.at[hg, got], ossem.at[0], orsem.at[hg, w],
                        device_id={'sp': nxt}, device_id_type=MESH).wait_recv()
            if w == 0:
                res[rows, :] += dot(orecv[hg, rows, :], wo[gw * hg:gw * hg + gw, :])
        if w == 1:
            r = res[rows, :]
            for hg in range(ng):
                r = r + dot(orecv[hg, rows, :], wo[gw * hg:gw * hg + gw, :])
            res[rows, :] = r
        y2[rows, :] = norm(res[rows, :], row(g2), row(be2)).astype(BF16)
        if w == 0:
            cp_w2.wait()
        for c in range(0, ff, 512):
            k = min(512, ff - c)
            h = dot(y2[rows, :], w1t[:, c:c + k]) + b1[pl.ds(c, k)].reshape(1, k)
            hid[rows, c:c + k] = gelu(h).astype(BF16)
        for j in range(0, d, 256):
            k = min(256, d - j)
            acc = res[rows, j:j + k] + dot(hid[rows, :], w2[:, j:j + k])
            acc = (acc + b2[pl.ds(j, k)].reshape(1, k)).astype(BF16)
            for p in range(lo, hi):
                out[tok * order[p]:tok * order[p] + tok, j:j + k] = acc[tok * (p - lo):tok * (p - lo) + tok, :]
            if w == 1:
                pltpu.make_async_copy(out.at[:, pl.ds(j, k)], out_hbm.at[:, pl.ds(j, k)], outsem.at[0]).start()
    wait_sent(1)

    @pl.when(core == 0)
    def _():
        forward_all(me + 1).wait_send()

    def drain(gs):
        rows = pl.ds(0, tok * (n - 1))
        for g in gs:
            pltpu.make_async_remote_copy(
                osend.at[g, rows], osend.at[0, rows], ossem.at[g], orsem.at[0, 0], device_id={'sp': nxt}, device_id_type=MESH).wait_send()

    drain((0, 1))

    @pl.when(core == 1)
    def _():
        drain((2, 3))

    pltpu.make_async_copy(out, out_hbm, outsem.at[0]).wait()


def solution(mesh):
    n = mesh.shape['sp']

    def device_step(images, w_patch, b_patch, pos_embed, ln1_gain, ln1_bias, w_qkv, b_qkv, w_out, b_out, ln2_gain, ln2_bias, w_fc1, b_fc1, w_fc2, b_fc2):
        nimg, rows, width, chans = images.shape
        tok, d = pos_embed.shape
        patch = w_patch.shape[0]
        _, _, heads, hd = w_qkv.shape
        ff = w_fc1.shape[1]
        m = nimg * tok
        ntok = n * tok
        cfg = (n, nimg, tok, d, heads, hd, ff, patch, chans)
        img_t = jnp.transpose(images, (0, 3, 1, 2))
        wp_t = jnp.transpose(w_patch, (0, 2, 1, 3))
        wqkv_t = jnp.transpose(w_qkv, (1, 2, 3, 0)).reshape(3 * d, d)
        wo_t = w_out.reshape(d, d)
        w1_t = jnp.transpose(w_fc1, (1, 0))

        hbm = pl.BlockSpec(memory_space=pltpu.HBM)
        V, S = pltpu.VMEM, pltpu.SemaphoreType.DMA
        out = pl.pallas_call(
            functools.partial(body, cfg),
            out_shape=jax.ShapeDtypeStruct((m, d), BF16),
            in_specs=[hbm] * 16,
            out_specs=hbm,
            scratch_shapes=[
                V((m, d), BF16),
                V(img_t.shape, F32), V(wp_t.shape, BF16), V((chans, 16, 16, d), BF16),
                V((4, 12 * hd, d), BF16), V((d, d), BF16), V((4, 512, d), BF16), V((d, ff), BF16), V((ff, d), BF16),
                V((d,), F32), V((tok, d), BF16), V((d,), F32), V((d,), F32), V((3, heads, hd), F32), V((d,), F32), V((d,), F32),
                V((d,), F32), V((ff,), F32), V((d,), F32),
                V((8 * chans, 16, width), F32), V((4 * tok, chans * 256), BF16),
                V((m, d), BF16), V((m, d), BF16), V((2, ntok, d), BF16),
                V((2, 12 * hd, ntok), F32), V((4, ntok, ntok), F32), V((4, ntok, ntok), BF16),
                V((3, 4, 8, hd), F32), V((4, 3, hd, 8), F32),
                V((4, ntok, 4 * hd), BF16), V((4, m, 4 * hd), BF16), V((m, d), F32), V((m, d), BF16), V((m, ff), BF16),
                S((1,)), S((2,)), S((2,)), S((1,)), S((4,)), S((4,)), S((10,)), S((2,)), S((n,)), S((1,)), S((1,)), S((4,)), S((4, 2)),
            ],
            compiler_params=pltpu.CompilerParams(collective_id=0, has_side_effects=True, vmem_limit_bytes=60 * 1024 * 1024),
            name='siglip_layer',
        )(img_t, wp_t, b_patch, pos_embed, ln1_gain, ln1_bias, wqkv_t, b_qkv, wo_t, b_out,
          ln2_gain, ln2_bias, w1_t, b_fc1, w_fc2, b_fc2)
        return out.reshape(nimg, tok, d)

    in_specs = (P('dp', 'sp', None, None), P(), P(), P('sp', None), P(), P(), P(), P(), P(), P(), P(), P(), P(), P(), P(), P())
    return jax.shard_map(device_step, mesh=mesh, in_specs=in_specs, out_specs=P('dp', 'sp', None), check_vma=False)
```

```python
import functools
import math

import jax
import jax.numpy as jnp
from jax import lax
from jax.experimental import pallas as pl
from jax.experimental.pallas import tpu as pltpu
from jax.sharding import PartitionSpec as P

LN_EPS = 1e-6
LOG2E = 1.4426950408889634
F32 = jnp.float32
BF16 = jnp.bfloat16
NT = (((1,), (1,)), ((), ()))
NN = (((1,), (0,)), ((), ()))
MESH = pl.DeviceIdType.MESH


def dot(a, b, dims=NN):
    return lax.dot_general(a, b, dims, preferred_element_type=F32)


def row(v):
    return v[...].reshape(1, v.shape[0])


def norm(z, gain, bias):
    mean = jnp.mean(z, axis=-1, keepdims=True)
    cen = z - mean
    var = jnp.mean(cen * cen, axis=-1, keepdims=True)
    return cen * lax.rsqrt(var + LN_EPS) * gain + bias


def gelu(x):
    inner = math.sqrt(2.0 / math.pi) * (x + 0.044715 * (x * x * x))
    return 0.5 * x * (1.0 + jnp.tanh(inner))


def chunk_transpose(w, chunk):
    rows, lanes = w.shape
    r = lax.broadcasted_iota(jnp.int32, w.shape, 0) % 8
    c = lax.broadcasted_iota(jnp.int32, w.shape, 1) // chunk
    for s in (4, 2, 1):
        up = pltpu.roll(pltpu.roll(w, s * chunk, 1), rows - s, 0)
        down = pltpu.roll(pltpu.roll(w, lanes - s * chunk, 1), s, 0)
        rb, cb = (r & s) != 0, (c & s) != 0
        w = jnp.where(rb == cb, w, jnp.where(cb, up, down))
    return w


def body(cfg, *refs):
    n, nimg, tok, d, heads, hd, ff, patch, chans = cfg
    (img_hbm, wp_hbm, bp_h, pos_h, g1_h, be1_h, wqkv_hbm, bqkv_h, wo_hbm, bo_h, g2_h, be2_h, w1_hbm, b1_h, w2_hbm, b2_h, out_hbm, out,
     img, wp_raw, wp, wq, wo, w1s, w1t, w2, bp, pos, g1, be1, bqkv, bo, g2, be2, b1, b2,
     zf, xs, x0, y1, yrecv, qkv, sbuf, pbuf, bsc, bcol, osend, orecv, res, y2, hid,
     outsem, isem, wsem, psem, qsem, csem, vsem, ssem, rsem, fsem, frsem, ossem, orsem) = refs
    ntok = n * tok
    gh, ng = 4, 3
    step, slots = w1s.shape[1], w1s.shape[0]
    gw = gh * hd
    me = lax.axis_index('sp')
    chip, core = me // 2, lax.rem(me, 2)
    pair, side = chip // 2, lax.rem(chip, 2)
    nxt = lax.rem(me + 1, n)
    pos_split, pos_full = pair, 2 + chip
    order = [i for i in range(nimg) if i % 3 == 1] + [i for i in range(nimg) if i % 3 != 1]

    def source_of(p, hg):
        return 2 * (2 * p + hg // 2) + 1 if p < 2 else 2 * (p - 2) + (hg == 0)

    def send_y(i, src_row, e, slot):
        return pltpu.make_async_remote_copy(
            y1.at[pl.ds(src_row, tok)], yrecv.at[0, pl.ds(pl.multiple_of(tok * slot, tok), tok)],
            ssem.at[i], rsem.at[slot], device_id={'sp': e}, device_id_type=MESH)

    def wait_sent(bi):
        for here in range(2):
            rows = pl.ds(0, tok * (n // 2 - (here != bi)))

            @pl.when(core == here)
            def _():
                pltpu.make_async_remote_copy(
                    yrecv.at[0, rows], yrecv.at[1, rows], ssem.at[bi], rsem.at[0], device_id={'sp': nxt}, device_id_type=MESH).wait_send()

    def forward(s, dst):
        rows = pl.ds(pl.multiple_of(tok * s, tok), tok)
        return pltpu.make_async_remote_copy(
            yrecv.at[0, rows], yrecv.at[1, rows], fsem.at[0], frsem.at[0], device_id={'sp': dst}, device_id_type=MESH)

    def forward_all(dst):
        return pltpu.make_async_remote_copy(
            yrecv.at[0], yrecv.at[1], fsem.at[0], frsem.at[0], device_id={'sp': dst}, device_id_type=MESH)

    def wave_of(g):
        return 1 - core if g < 2 else 1

    def send_o(g, s, hg, i):
        return pltpu.make_async_remote_copy(
            osend.at[g, pl.ds(pl.multiple_of(tok * s, tok), tok)], orecv.at[hg, pl.ds(pl.multiple_of(tok * i, tok), tok)],
            ossem.at[g], orsem.at[hg, wave_of(g)], device_id={'sp': s}, device_id_type=MESH)

    def head_group(g):
        return (1 - core) * (g + 1) + core * (2 * side + g) if g < 2 else (1 - core) * (g + 1)

    def w1_copy(c, slot, size):
        start = c * step if isinstance(c, int) else pl.multiple_of(c * step, step)
        return pltpu.make_async_copy(w1_hbm.at[pl.ds(start, size)], w1s.at[slot, pl.ds(0, size)], csem.at[slot])

    batches = (order[:2], order[2:])
    bounds = (0, 2, nimg)
    cp_img = [pltpu.make_async_copy(img_hbm.at[i], img.at[i], isem.at[0 if i in order[:2] else 1]) for i in range(nimg)]
    cp_wp = [pltpu.make_async_copy(wp_hbm, wp_raw, psem.at[0])]
    cp_wo = pltpu.make_async_copy(wo_hbm, wo, wsem.at[0])
    cp_w2 = pltpu.make_async_copy(w2_hbm, w2, wsem.at[1])
    cp_q = [pltpu.make_async_copy(
        wqkv_hbm.at[pl.ds(pl.multiple_of(d * t + gw * head_group(g), 32), gw)], wq.at[g, pl.ds(gw * t, gw)], qsem.at[g])
        for g in range(ng) for t in range(3)]
    cp_v = [pltpu.make_async_copy(a, b, vsem.at[k]) for k, (a, b) in enumerate(
        ((bp_h, bp), (pos_h, pos), (g1_h, g1), (be1_h, be1), (bqkv_h, bqkv), (bo_h, bo), (g2_h, g2), (be2_h, be2), (b1_h, b1), (b2_h, b2)))]
    for c in cp_wp + [cp_img[i] for i in batches[0]] + cp_v[:4] + [cp_img[i] for i in batches[1]] + cp_v[4:]:
        c.start()
    wp[...] = jnp.zeros_like(wp)
    barrier = pltpu.get_barrier_semaphore()
    for k in range(1, n):
        pl.semaphore_signal(barrier, inc=1, device_id={'sp': lax.rem(me + k, n)}, device_id_type=MESH)

    zf[...] = jnp.zeros_like(zf)
    lrow = lax.broadcasted_iota(jnp.int32, (224, 256), 0)
    lcol = lax.broadcasted_iota(jnp.int32, (224, 256), 1)
    sel = jnp.where((lcol % 16 < patch) & (lrow == patch * (lcol // 16) + lcol % 16), 1.0, 0.0).astype(BF16)

    full, early = ff // step, 3
    rest = ff - full * step

    def turn(c, size, slot):
        w1t[:, pl.ds(c * step if isinstance(c, int) else pl.multiple_of(c * step, step), size)] = jnp.transpose(w1s[slot, 0:size])

    def turn_step(c, carry):
        slot = lax.rem(c, slots)
        w1_copy(c, slot, step).wait()
        turn(c, step, slot)

        @pl.when(c + slots < full)
        def _():
            w1_copy(c + slots, slot, step).start()

        @pl.when(c + slots == full)
        def _():
            w1_copy(full, slot, rest).start()

        return carry

    for bi, batch in enumerate(batches):
        nb = len(batch)
        pltpu.make_async_copy(img_hbm.at[pl.ds(0, nb)], img.at[pl.ds(0, nb)], isem.at[bi]).wait()
        if bi == len(batches) - 1:
            for c in cp_q:
                c.start()
        for b, i in enumerate(batch):
            for y in range(2):
                for c in range(chans):
                    zf[(b * 2 + y) * chans + c, 0:patch, :] = img[i, c, patch * y:patch * y + patch, :]
        nz = nb * 2 * chans
        u = dot(zf[0:nz].reshape(nz * 16, 224).astype(BF16), sel)
        u = u.reshape(nz, 2, 8, 256)
        for ph in range(2):
            parts = []
            for xh in range(2):
                blk = u[:, ph, :, 128 * xh:128 * xh + 128].reshape(nz * 8, 128)
                parts.append(chunk_transpose(blk, 16).reshape(nz, 1, 8, 128))
            t = jnp.concatenate(parts, axis=1).reshape(nb * 2, chans, 16, 128).astype(BF16)
            for c in range(chans):
                xs[0:nb * tok, 256 * c + 128 * ph:256 * c + 128 * ph + 128] = t[:, c].reshape(nb * tok, 128)
        if bi == 0:
            for c in cp_wp + cp_v[:4]:
                c.wait()
            for c in range(slots):
                w1_copy(c, c, step).start()
            for c in range(chans):
                for p in range(patch):
                    wp[c, p, 0:patch, :] = wp_raw[p, c]
        e = dot(xs[0:nb * tok, :], wp[...].reshape(chans * 256, d))
        base = row(bp) + pos[...].astype(F32)
        xb = (e + jnp.concatenate([base] * nb, axis=0)).astype(BF16)
        yb = norm(xb.astype(F32), row(g1), row(be1)).astype(BF16)
        x0[tok * bounds[bi]:tok * bounds[bi + 1], :] = xb
        y1[tok * bounds[bi]:tok * bounds[bi + 1], :] = yb
        if bi == 0:
            pl.semaphore_wait(barrier, n - 1)
        if bi == 1:
            lax.fori_loop(0, early, turn_step, 0)
            wait_sent(0)
        for k in (2, 1, 3, 0):
            c = lax.rem(chip + k, n // 2)
            if bi == 0:
                e, p = 2 * c + 1, c // 2
            else:
                e, p = 2 * c, 2 + c
            src = pl.multiple_of(tok * p, tok)

            @pl.when(me != e)
            def _():
                send_y(bi, src, e, me).start()

            @pl.when(me == e)
            def _():
                yrecv[0, pl.ds(pl.multiple_of(tok * me, tok), tok), :] = y1[pl.ds(src, tok), :]

    for c in cp_v[4:]:
        c.wait()
    for t in range(3):
        for hg in range(heads // gh):
            bsc[t, hg, 0:gh, :] = bqkv[t, gh * hg:gh * hg + gh, :]
    for g in range(ng):
        for t in range(3):
            col = jnp.transpose(bsc[t, head_group(g)])
            for j in range(gh):
                bcol[g, gw * t + hd * j:gw * t + hd * j + hd, :] = jnp.broadcast_to(col[:, j:j + 1], (hd, 128))
    res[...] = x0[...].astype(F32) + row(bo)
    lax.fori_loop(early, full, turn_step, 0)

    cp_wo.start()
    cp_w2.start()
    w1_copy(full, full % slots, rest).wait()
    turn(full, rest, full % slots)

    def project(g, slot, parts):
        for t in parts:
            qkv[g % 2, gw * t:gw * t + gw, :] = dot(wq[g, gw * t:gw * t + gw, :], yrecv[slot], NT)

    def head(g, t, j):
        part = slice(gw * t + hd * j, gw * t + hd * j + hd)
        return qkv[g % 2, part, :] + jnp.concatenate([bcol[g, part, :]] * (ntok // 128), axis=1)

    def scores(g, j):
        sbuf[g % 2, j] = dot(jnp.transpose(head(g, 1, j)).astype(BF16), head(g, 0, j).astype(BF16))

    def soft(g, j):
        for b in range(0, ntok, 128):
            s = sbuf[g % 2, j, :, b:b + 128]
            p = jnp.exp2((s - jnp.max(s, axis=0, keepdims=True)) * (hd ** -0.5 * LOG2E))
            pbuf[g % 2, j, :, b:b + 128] = (p * (1.0 / jnp.sum(p, axis=0, keepdims=True))).astype(BF16)

    def mix(g, j):
        return dot(head(g, 2, j).astype(BF16), pbuf[g % 2, j])

    def wait_q(g):
        pltpu.make_async_copy(wqkv_hbm.at[pl.ds(0, 3 * gw)], wq.at[g], qsem.at[g]).wait()

    def run_groups(gs, slot, i):
        for g in gs:
            wait_q(g)
        project(gs[0], slot, range(3))
        for g in gs:
            for j in range(gh):
                scores(g, j)
            outs = []
            for j in range(gh):
                if g + 1 in gs and j < 3:
                    project(g + 1, slot, (j,))
                soft(g, j)
                if j:
                    outs.append(mix(g, j - 1))
            outs.append(mix(g, gh - 1))
            osend[g] = jnp.transpose(jnp.concatenate(outs, axis=0)).astype(BF16)
            hg = head_group(g)
            for k in (4, 5, 3, 2, 6, 7, 1):
                send_o(g, lax.rem(me + k, n), hg, i).start()
            orecv[hg, pl.ds(pl.multiple_of(tok * i, tok), tok), :] = osend[g, pl.ds(pl.multiple_of(tok * me, tok), tok), :]


    @pl.when(core == 0)
    def _():
        for k in (0, 1, 2, 3, 6, 7, 4, 5):
            s = lax.rem(me + k, n)
            if k:
                send_y(0, 0, s, s).wait_recv()
            forward(s, me + 1).start()
        run_groups((0, 1, 2), 0, pos_full)

    @pl.when(core == 1)
    def _():
        for k in range(1, n):
            s = lax.rem(me + k, n)
            send_y(0, 0, s, s).wait_recv()
        run_groups((0, 1), 0, pos_split)
        forward_all(me - 1).wait_recv()
        run_groups((2,), 1, pos_full)

    cp_wo.wait()
    cp_w2.wait()
    def recv_o(w, hg):
        lo, hi = bounds[w], bounds[w + 1]
        mine = sum(jnp.where(me == source_of(p, hg), 1, 0) for p in range(lo, hi))
        for k in range(2):
            got = pl.ds(0, tok * (hi - lo - k))

            @pl.when(mine == k)
            def _():
                pltpu.make_async_remote_copy(
                    osend.at[0, got], orecv.at[hg, got], ossem.at[0], orsem.at[hg, w],
                    device_id={'sp': nxt}, device_id_type=MESH).wait_recv()

    def join(w, hgs):
        rows = slice(tok * bounds[w], tok * bounds[w + 1])
        r = res[rows, :]
        for hg in hgs:
            r = r + dot(orecv[hg, rows, :], wo[gw * hg:gw * hg + gw, :])
        res[rows, :] = r

    def expand(w):
        rows = slice(tok * bounds[w], tok * bounds[w + 1])
        y2[rows, :] = norm(res[rows, :], row(g2), row(be2)).astype(BF16)
        for c in range(0, ff, 512):
            k = min(512, ff - c)
            h = dot(y2[rows, :], w1t[:, c:c + k]) + b1[pl.ds(c, k)].reshape(1, k)
            hid[rows, c:c + k] = gelu(h).astype(BF16)

    def contract(w):
        lo, hi = bounds[w], bounds[w + 1]
        rows = slice(tok * lo, tok * hi)
        for j in range(0, d, 256):
            k = min(256, d - j)
            acc = res[rows, j:j + k] + dot(hid[rows, :], w2[:, j:j + k])
            acc = (acc + b2[pl.ds(j, k)].reshape(1, k)).astype(BF16)
            for p in range(lo, hi):
                out[tok * order[p]:tok * order[p] + tok, j:j + k] = acc[tok * (p - lo):tok * (p - lo) + tok, :]
            if w == 1:
                pltpu.make_async_copy(out.at[:, pl.ds(j, k)], out_hbm.at[:, pl.ds(j, k)], outsem.at[0]).start()

    for w in range(2):
        for hg in ((0, 2, 1, 3), (1, 0, 2, 3))[w]:
            recv_o(w, hg)
        join(w, range(4))
        expand(w)
        contract(w)
    wait_sent(1)

    @pl.when(core == 0)
    def _():
        forward_all(me + 1).wait_send()

    def drain(gs):
        rows = pl.ds(0, tok * (n - 1))
        for g in gs:
            pltpu.make_async_remote_copy(
                osend.at[g, rows], osend.at[0, rows], ossem.at[g], orsem.at[0, 0], device_id={'sp': nxt}, device_id_type=MESH).wait_send()

    drain(range(ng))

    pltpu.make_async_copy(out, out_hbm, outsem.at[0]).wait()


def solution(mesh):
    n = mesh.shape['sp']

    def device_step(images, w_patch, b_patch, pos_embed, ln1_gain, ln1_bias, w_qkv, b_qkv, w_out, b_out, ln2_gain, ln2_bias, w_fc1, b_fc1, w_fc2, b_fc2):
        nimg, rows, width, chans = images.shape
        tok, d = pos_embed.shape
        patch = w_patch.shape[0]
        _, _, heads, hd = w_qkv.shape
        ff = w_fc1.shape[1]
        m = nimg * tok
        ntok = n * tok
        cfg = (n, nimg, tok, d, heads, hd, ff, patch, chans)
        img_t = jnp.transpose(images, (0, 3, 1, 2))
        wp_t = jnp.transpose(w_patch, (0, 2, 1, 3))
        wqkv_t = jnp.transpose(w_qkv, (1, 2, 3, 0)).reshape(3 * d, d)
        wo_t = w_out.reshape(d, d)
        w1_t = jnp.transpose(w_fc1, (1, 0))

        hbm = pl.BlockSpec(memory_space=pltpu.HBM)
        V, S = pltpu.VMEM, pltpu.SemaphoreType.DMA
        out = pl.pallas_call(
            functools.partial(body, cfg),
            out_shape=jax.ShapeDtypeStruct((m, d), BF16),
            in_specs=[hbm] * 16,
            out_specs=hbm,
            scratch_shapes=[
                V((m, d), BF16),
                V(img_t.shape, F32), V(wp_t.shape, BF16), V((chans, 16, 16, d), BF16),
                V((3, 12 * hd, d), BF16), V((d, d), BF16), V((4, 512, d), BF16), V((d, ff), BF16), V((ff, d), BF16),
                V((d,), F32), V((tok, d), BF16), V((d,), F32), V((d,), F32), V((3, heads, hd), F32), V((d,), F32), V((d,), F32),
                V((d,), F32), V((ff,), F32), V((d,), F32),
                V((8 * chans, 16, width), F32), V((4 * tok, chans * 256), BF16),
                V((m, d), BF16), V((m, d), BF16), V((2, ntok, d), BF16),
                V((2, 12 * hd, ntok), F32), V((2, 4, ntok, ntok), F32), V((2, 4, ntok, ntok), BF16),
                V((3, 4, 8, hd), F32), V((3, 12 * hd, 128), F32),
                V((3, ntok, 4 * hd), BF16), V((4, m, 4 * hd), BF16), V((m, d), F32), V((m, d), BF16), V((m, ff), BF16),
                S((1,)), S((2,)), S((2,)), S((1,)), S((3,)), S((4,)), S((10,)), S((2,)), S((n,)), S((1,)), S((1,)), S((3,)), S((4, 2)),
            ],
            compiler_params=pltpu.CompilerParams(collective_id=0, has_side_effects=True, vmem_limit_bytes=60 * 1024 * 1024),
            name='siglip_layer',
        )(img_t, wp_t, b_patch, pos_embed, ln1_gain, ln1_bias, wqkv_t, b_qkv, wo_t, b_out,
          ln2_gain, ln2_bias, w1_t, b_fc1, w_fc2, b_fc2)
        return out.reshape(nimg, tok, d)

    in_specs = (P('dp', 'sp', None, None), P(), P(), P('sp', None), P(), P(), P(), P(), P(), P(), P(), P(), P(), P(), P(), P())
    return jax.shard_map(device_step, mesh=mesh, in_specs=in_specs, out_specs=P('dp', 'sp', None), check_vma=False)
```

```python
import functools
import math

import jax
import jax.numpy as jnp
from jax import lax
from jax.experimental import pallas as pl
from jax.experimental.pallas import tpu as pltpu
from jax.sharding import PartitionSpec as P

LN_EPS = 1e-6
LOG2E = 1.4426950408889634
F32 = jnp.float32
BF16 = jnp.bfloat16
NT = (((1,), (1,)), ((), ()))
NN = (((1,), (0,)), ((), ()))
MESH = pl.DeviceIdType.MESH


def dot(a, b, dims=NN):
    return lax.dot_general(a, b, dims, preferred_element_type=F32)


def row(v):
    return v[...].reshape(1, v.shape[0])


def norm(z, gain, bias):
    mean = jnp.mean(z, axis=-1, keepdims=True)
    cen = z - mean
    var = jnp.mean(cen * cen, axis=-1, keepdims=True)
    return cen * lax.rsqrt(var + LN_EPS) * gain + bias


def gelu(x):
    inner = math.sqrt(2.0 / math.pi) * (x + 0.044715 * (x * x * x))
    return 0.5 * x * (1.0 + jnp.tanh(inner))


def chunk_transpose(w, chunk):
    rows, lanes = w.shape
    r = lax.broadcasted_iota(jnp.int32, w.shape, 0) % 8
    c = lax.broadcasted_iota(jnp.int32, w.shape, 1) // chunk
    for s in (4, 2, 1):
        up = pltpu.roll(pltpu.roll(w, s * chunk, 1), rows - s, 0)
        down = pltpu.roll(pltpu.roll(w, lanes - s * chunk, 1), s, 0)
        rb, cb = (r & s) != 0, (c & s) != 0
        w = jnp.where(rb == cb, w, jnp.where(cb, up, down))
    return w


def body(cfg, *refs):
    n, nimg, tok, d, heads, hd, ff, patch, chans = cfg
    (img_hbm, wp_hbm, bp_h, pos_h, g1_h, be1_h, wqkv_hbm, bqkv_h, wo_hbm, bo_h, g2_h, be2_h, w1_hbm, b1_h, w2_hbm, b2_h, out_hbm, out,
     img, wp_raw, wp, wq, wo, w1s, w1t, w2, bp, pos, g1, be1, bqkv, bo, g2, be2, b1, b2,
     zf, xs, x0, y1, yrecv, qkv, sbuf, pbuf, bsc, bcol, osend, orecv, res, y2, hid,
     outsem, isem, wsem, psem, qsem, csem, vsem, ssem, rsem, fsem, frsem, ossem, orsem) = refs
    ntok = n * tok
    gh, ng = 4, 3
    step, slots = w1s.shape[1], w1s.shape[0]
    gw = gh * hd
    me = lax.axis_index('sp')
    chip, core = me // 2, lax.rem(me, 2)
    pair, side = chip // 2, lax.rem(chip, 2)
    nxt = lax.rem(me + 1, n)
    pos_split, pos_full = pair, 2 + chip
    order = [i for i in range(nimg) if i % 3 == 1] + [i for i in range(nimg) if i % 3 != 1]

    def source_of(p, hg):
        return 2 * (2 * p + hg // 2) + 1 if p < 2 else 2 * (p - 2) + (hg == 0)

    def send_y(i, src_row, e, slot):
        return pltpu.make_async_remote_copy(
            y1.at[pl.ds(src_row, tok)], yrecv.at[0, pl.ds(pl.multiple_of(tok * slot, tok), tok)],
            ssem.at[i], rsem.at[slot], device_id={'sp': e}, device_id_type=MESH)

    def wait_sent(bi):
        for here in range(2):
            rows = pl.ds(0, tok * (n // 2 - (here != bi)))

            @pl.when(core == here)
            def _():
                pltpu.make_async_remote_copy(
                    yrecv.at[0, rows], yrecv.at[1, rows], ssem.at[bi], rsem.at[0], device_id={'sp': nxt}, device_id_type=MESH).wait_send()

    def forward(s, dst):
        rows = pl.ds(pl.multiple_of(tok * s, tok), tok)
        return pltpu.make_async_remote_copy(
            yrecv.at[0, rows], yrecv.at[1, rows], fsem.at[0], frsem.at[0], device_id={'sp': dst}, device_id_type=MESH)

    def forward_all(dst):
        return pltpu.make_async_remote_copy(
            yrecv.at[0], yrecv.at[1], fsem.at[0], frsem.at[0], device_id={'sp': dst}, device_id_type=MESH)

    def wave_of(g):
        return 1 - core if g < 2 else 1

    def send_o(g, s, hg, i):
        return pltpu.make_async_remote_copy(
            osend.at[g, pl.ds(pl.multiple_of(tok * s, tok), tok)], orecv.at[hg, pl.ds(pl.multiple_of(tok * i, tok), tok)],
            ossem.at[g], orsem.at[hg, wave_of(g)], device_id={'sp': s}, device_id_type=MESH)

    def head_group(g):
        return (1 - core) * (g + 1) + core * (2 * side + g) if g < 2 else (1 - core) * (g + 1)

    def w1_copy(c, slot, size):
        start = c * step if isinstance(c, int) else pl.multiple_of(c * step, step)
        return pltpu.make_async_copy(w1_hbm.at[pl.ds(start, size)], w1s.at[slot, pl.ds(0, size)], csem.at[slot])

    batches = (order[:2], order[2:])
    bounds = (0, 2, nimg)
    cp_img = [pltpu.make_async_copy(img_hbm.at[i], img.at[i], isem.at[0 if i in order[:2] else 1]) for i in range(nimg)]
    cp_wp = [pltpu.make_async_copy(wp_hbm, wp_raw, psem.at[0])]
    cp_wo = pltpu.make_async_copy(wo_hbm, wo, wsem.at[0])
    cp_w2 = pltpu.make_async_copy(w2_hbm, w2, wsem.at[1])
    cp_q = [pltpu.make_async_copy(
        wqkv_hbm.at[pl.ds(pl.multiple_of(d * t + gw * head_group(g), 32), gw)], wq.at[g, pl.ds(gw * t, gw)], qsem.at[g])
        for g in range(ng) for t in range(3)]
    cp_v = [pltpu.make_async_copy(a, b, vsem.at[k]) for k, (a, b) in enumerate(
        ((bp_h, bp), (pos_h, pos), (g1_h, g1), (be1_h, be1), (bqkv_h, bqkv), (bo_h, bo), (g2_h, g2), (be2_h, be2), (b1_h, b1), (b2_h, b2)))]
    for c in cp_wp + [cp_img[i] for i in batches[0]] + cp_v[:4] + [cp_img[i] for i in batches[1]] + cp_v[4:]:
        c.start()
    wp[...] = jnp.zeros_like(wp)
    barrier = pltpu.get_barrier_semaphore()
    for k in range(1, n):
        pl.semaphore_signal(barrier, inc=1, device_id={'sp': lax.rem(me + k, n)}, device_id_type=MESH)

    zf[...] = jnp.zeros_like(zf)
    lrow = lax.broadcasted_iota(jnp.int32, (224, 256), 0)
    lcol = lax.broadcasted_iota(jnp.int32, (224, 256), 1)
    sel = jnp.where((lcol % 16 < patch) & (lrow == patch * (lcol // 16) + lcol % 16), 1.0, 0.0).astype(BF16)

    full, early = ff // step, 3
    rest = ff - full * step

    def turn(c, size, slot):
        w1t[:, pl.ds(c * step if isinstance(c, int) else pl.multiple_of(c * step, step), size)] = jnp.transpose(w1s[slot, 0:size])

    def turn_step(c, carry):
        slot = lax.rem(c, slots)
        w1_copy(c, slot, step).wait()
        turn(c, step, slot)

        @pl.when(c + slots < full)
        def _():
            w1_copy(c + slots, slot, step).start()

        @pl.when(c + slots == full)
        def _():
            w1_copy(full, slot, rest).start()

        return carry

    for bi, batch in enumerate(batches):
        nb = len(batch)
        pltpu.make_async_copy(img_hbm.at[pl.ds(0, nb)], img.at[pl.ds(0, nb)], isem.at[bi]).wait()
        if bi == len(batches) - 1:
            for c in cp_q:
                c.start()
        for b, i in enumerate(batch):
            for y in range(2):
                for c in range(chans):
                    zf[(b * 2 + y) * chans + c, 0:patch, :] = img[i, c, patch * y:patch * y + patch, :]
        nz = nb * 2 * chans
        u = dot(zf[0:nz].reshape(nz * 16, 224).astype(BF16), sel)
        u = u.reshape(nz, 2, 8, 256)
        for ph in range(2):
            parts = []
            for xh in range(2):
                blk = u[:, ph, :, 128 * xh:128 * xh + 128].reshape(nz * 8, 128)
                parts.append(chunk_transpose(blk, 16).reshape(nz, 1, 8, 128))
            t = jnp.concatenate(parts, axis=1).reshape(nb * 2, chans, 16, 128).astype(BF16)
            for c in range(chans):
                xs[0:nb * tok, 256 * c + 128 * ph:256 * c + 128 * ph + 128] = t[:, c].reshape(nb * tok, 128)
        if bi == 0:
            for c in cp_wp + cp_v[:4]:
                c.wait()
            for c in range(slots):
                w1_copy(c, c, step).start()
            for c in range(chans):
                for p in range(patch):
                    wp[c, p, 0:patch, :] = wp_raw[p, c]
        e = dot(xs[0:nb * tok, :], wp[...].reshape(chans * 256, d))
        base = row(bp) + pos[...].astype(F32)
        xb = (e + jnp.concatenate([base] * nb, axis=0)).astype(BF16)
        yb = norm(xb.astype(F32), row(g1), row(be1)).astype(BF16)
        x0[tok * bounds[bi]:tok * bounds[bi + 1], :] = xb
        y1[tok * bounds[bi]:tok * bounds[bi + 1], :] = yb
        if bi == 0:
            pl.semaphore_wait(barrier, n - 1)
        if bi == 1:
            lax.fori_loop(0, early, turn_step, 0)
        for k in (2, 1, 3, 0):
            c = lax.rem(chip + k, n // 2)
            if bi == 0:
                e, p = 2 * c + 1, c // 2
            else:
                e, p = 2 * c, 2 + c
            src = pl.multiple_of(tok * p, tok)

            @pl.when(me != e)
            def _():
                send_y(bi, src, e, me).start()

            @pl.when(me == e)
            def _():
                yrecv[0, pl.ds(pl.multiple_of(tok * me, tok), tok), :] = y1[pl.ds(src, tok), :]

    for c in cp_v[4:]:
        c.wait()
    for t in range(3):
        for hg in range(heads // gh):
            bsc[t, hg, 0:gh, :] = bqkv[t, gh * hg:gh * hg + gh, :]
    for g in range(ng):
        for t in range(3):
            col = jnp.transpose(bsc[t, head_group(g)])
            for j in range(gh):
                bcol[g, gw * t + hd * j:gw * t + hd * j + hd, :] = jnp.broadcast_to(col[:, j:j + 1], (hd, 128))
    res[...] = x0[...].astype(F32) + row(bo)
    lax.fori_loop(early, full, turn_step, 0)

    cp_wo.start()
    cp_w2.start()
    w1_copy(full, full % slots, rest).wait()
    turn(full, rest, full % slots)

    def project(g, slot, parts):
        for t in parts:
            qkv[g % 2, gw * t:gw * t + gw, :] = dot(wq[g, gw * t:gw * t + gw, :], yrecv[slot], NT)

    def head(g, t, j):
        part = slice(gw * t + hd * j, gw * t + hd * j + hd)
        return qkv[g % 2, part, :] + jnp.concatenate([bcol[g, part, :]] * (ntok // 128), axis=1)

    def scores(g, j):
        sbuf[g % 2, j] = dot(jnp.transpose(head(g, 1, j)).astype(BF16), head(g, 0, j).astype(BF16))

    def soft(g, j):
        for b in range(0, ntok, 128):
            s = sbuf[g % 2, j, :, b:b + 128]
            p = jnp.exp2((s - jnp.max(s, axis=0, keepdims=True)) * (hd ** -0.5 * LOG2E))
            pbuf[g % 2, j, :, b:b + 128] = (p * (1.0 / jnp.sum(p, axis=0, keepdims=True))).astype(BF16)

    def mix(g, j):
        return dot(head(g, 2, j).astype(BF16), pbuf[g % 2, j])

    def wait_q(g):
        pltpu.make_async_copy(wqkv_hbm.at[pl.ds(0, 3 * gw)], wq.at[g], qsem.at[g]).wait()

    def run_groups(gs, slot, i):
        for g in gs:
            wait_q(g)
        project(gs[0], slot, range(3))
        for g in gs:
            for j in range(gh):
                scores(g, j)
            outs = []
            for j in range(gh):
                if g + 1 in gs and j < 3:
                    project(g + 1, slot, (j,))
                soft(g, j)
                if j:
                    outs.append(mix(g, j - 1))
            outs.append(mix(g, gh - 1))
            osend[g] = jnp.transpose(jnp.concatenate(outs, axis=0)).astype(BF16)
            hg = head_group(g)
            for k in (4, 5, 3, 2, 6, 7, 1):
                send_o(g, lax.rem(me + k, n), hg, i).start()
            orecv[hg, pl.ds(pl.multiple_of(tok * i, tok), tok), :] = osend[g, pl.ds(pl.multiple_of(tok * me, tok), tok), :]


    @pl.when(core == 0)
    def _():
        for k in (0, 1, 2, 3, 6, 7, 4, 5):
            s = lax.rem(me + k, n)
            if k:
                send_y(0, 0, s, s).wait_recv()
            forward(s, me + 1).start()
        run_groups((0, 1, 2), 0, pos_full)

    @pl.when(core == 1)
    def _():
        for k in range(1, n):
            s = lax.rem(me + k, n)
            send_y(0, 0, s, s).wait_recv()
        run_groups((0, 1), 0, pos_split)
        forward_all(me - 1).wait_recv()
        run_groups((2,), 1, pos_full)

    cp_wo.wait()
    cp_w2.wait()
    def recv_o(w, hg):
        lo, hi = bounds[w], bounds[w + 1]
        mine = sum(jnp.where(me == source_of(p, hg), 1, 0) for p in range(lo, hi))
        for k in range(2):
            got = pl.ds(0, tok * (hi - lo - k))

            @pl.when(mine == k)
            def _():
                pltpu.make_async_remote_copy(
                    osend.at[0, got], orecv.at[hg, got], ossem.at[0], orsem.at[hg, w],
                    device_id={'sp': nxt}, device_id_type=MESH).wait_recv()

    def join(w, hgs):
        rows = slice(tok * bounds[w], tok * bounds[w + 1])
        o = jnp.concatenate([orecv[hg, rows, :] for hg in hgs], axis=1)
        res[rows, :] += dot(o, wo[...])

    def expand(w):
        rows = slice(tok * bounds[w], tok * bounds[w + 1])
        y2[rows, :] = norm(res[rows, :], row(g2), row(be2)).astype(BF16)
        for c in range(0, ff, 512):
            k = min(512, ff - c)
            h = dot(y2[rows, :], w1t[:, c:c + k]) + b1[pl.ds(c, k)].reshape(1, k)
            hid[rows, c:c + k] = gelu(h).astype(BF16)

    def contract(w):
        lo, hi = bounds[w], bounds[w + 1]
        rows = slice(tok * lo, tok * hi)
        for j in range(0, d, 256):
            k = min(256, d - j)
            acc = res[rows, j:j + k] + dot(hid[rows, :], w2[:, j:j + k])
            acc = (acc + b2[pl.ds(j, k)].reshape(1, k)).astype(BF16)
            for p in range(lo, hi):
                out[tok * order[p]:tok * order[p] + tok, j:j + k] = acc[tok * (p - lo):tok * (p - lo) + tok, :]
            if w == 1:
                pltpu.make_async_copy(out.at[:, pl.ds(j, k)], out_hbm.at[:, pl.ds(j, k)], outsem.at[0]).start()

    for w in range(2):
        for hg in ((0, 2, 1, 3), (1, 0, 2, 3))[w]:
            recv_o(w, hg)
        join(w, range(4))
        expand(w)
        contract(w)
    wait_sent(0)
    wait_sent(1)

    @pl.when(core == 0)
    def _():
        forward_all(me + 1).wait_send()

    def drain(gs):
        rows = pl.ds(0, tok * (n - 1))
        for g in gs:
            pltpu.make_async_remote_copy(
                osend.at[g, rows], osend.at[0, rows], ossem.at[g], orsem.at[0, 0], device_id={'sp': nxt}, device_id_type=MESH).wait_send()

    drain(range(ng))

    pltpu.make_async_copy(out, out_hbm, outsem.at[0]).wait()


def solution(mesh):
    n = mesh.shape['sp']

    def device_step(images, w_patch, b_patch, pos_embed, ln1_gain, ln1_bias, w_qkv, b_qkv, w_out, b_out, ln2_gain, ln2_bias, w_fc1, b_fc1, w_fc2, b_fc2):
        nimg, rows, width, chans = images.shape
        tok, d = pos_embed.shape
        patch = w_patch.shape[0]
        _, _, heads, hd = w_qkv.shape
        ff = w_fc1.shape[1]
        m = nimg * tok
        ntok = n * tok
        cfg = (n, nimg, tok, d, heads, hd, ff, patch, chans)
        img_t = jnp.transpose(images, (0, 3, 1, 2))
        wp_t = jnp.transpose(w_patch, (0, 2, 1, 3))
        wqkv_t = jnp.transpose(w_qkv, (1, 2, 3, 0)).reshape(3 * d, d)
        wo_t = w_out.reshape(d, d)
        w1_t = jnp.transpose(w_fc1, (1, 0))

        hbm = pl.BlockSpec(memory_space=pltpu.HBM)
        V, S = pltpu.VMEM, pltpu.SemaphoreType.DMA
        out = pl.pallas_call(
            functools.partial(body, cfg),
            out_shape=jax.ShapeDtypeStruct((m, d), BF16),
            in_specs=[hbm] * 16,
            out_specs=hbm,
            scratch_shapes=[
                V((m, d), BF16),
                V(img_t.shape, F32), V(wp_t.shape, BF16), V((chans, 16, 16, d), BF16),
                V((3, 12 * hd, d), BF16), V((d, d), BF16), V((4, 512, d), BF16), V((d, ff), BF16), V((ff, d), BF16),
                V((d,), F32), V((tok, d), BF16), V((d,), F32), V((d,), F32), V((3, heads, hd), F32), V((d,), F32), V((d,), F32),
                V((d,), F32), V((ff,), F32), V((d,), F32),
                V((8 * chans, 16, width), F32), V((4 * tok, chans * 256), BF16),
                V((m, d), BF16), V((m, d), BF16), V((2, ntok, d), BF16),
                V((2, 12 * hd, ntok), F32), V((2, 4, ntok, ntok), F32), V((2, 4, ntok, ntok), BF16),
                V((3, 4, 8, hd), F32), V((3, 12 * hd, 128), F32),
                V((3, ntok, 4 * hd), BF16), V((4, m, 4 * hd), BF16), V((m, d), F32), V((m, d), BF16), V((m, ff), BF16),
                S((1,)), S((2,)), S((2,)), S((1,)), S((3,)), S((4,)), S((10,)), S((2,)), S((n,)), S((1,)), S((1,)), S((3,)), S((4, 2)),
            ],
            compiler_params=pltpu.CompilerParams(collective_id=0, has_side_effects=True, vmem_limit_bytes=60 * 1024 * 1024),
            name='siglip_layer',
        )(img_t, wp_t, b_patch, pos_embed, ln1_gain, ln1_bias, wqkv_t, b_qkv, wo_t, b_out,
          ln2_gain, ln2_bias, w1_t, b_fc1, w_fc2, b_fc2)
        return out.reshape(nimg, tok, d)

    in_specs = (P('dp', 'sp', None, None), P(), P(), P('sp', None), P(), P(), P(), P(), P(), P(), P(), P(), P(), P(), P(), P())
    return jax.shard_map(device_step, mesh=mesh, in_specs=in_specs, out_specs=P('dp', 'sp', None), check_vma=False)
```

```python
import functools
import math

import jax
import jax.numpy as jnp
from jax import lax
from jax.experimental import pallas as pl
from jax.experimental.pallas import tpu as pltpu
from jax.sharding import PartitionSpec as P

LN_EPS = 1e-6
LOG2E = 1.4426950408889634
F32 = jnp.float32
BF16 = jnp.bfloat16
NT = (((1,), (1,)), ((), ()))
NN = (((1,), (0,)), ((), ()))
MESH = pl.DeviceIdType.MESH


def dot(a, b, dims=NN):
    return lax.dot_general(a, b, dims, preferred_element_type=F32)


def row(v):
    return v[...].reshape(1, v.shape[0])


def norm(z, gain, bias):
    mean = jnp.mean(z, axis=-1, keepdims=True)
    cen = z - mean
    var = jnp.mean(cen * cen, axis=-1, keepdims=True)
    return cen * lax.rsqrt(var + LN_EPS) * gain + bias


def gelu(x):
    inner = math.sqrt(2.0 / math.pi) * (x + 0.044715 * (x * x * x))
    return 0.5 * x * (1.0 + jnp.tanh(inner))


def chunk_transpose(w, chunk):
    rows, lanes = w.shape
    r = lax.broadcasted_iota(jnp.int32, w.shape, 0) % 8
    c = lax.broadcasted_iota(jnp.int32, w.shape, 1) // chunk
    for s in (4, 2, 1):
        up = pltpu.roll(pltpu.roll(w, s * chunk, 1), rows - s, 0)
        down = pltpu.roll(pltpu.roll(w, lanes - s * chunk, 1), s, 0)
        rb, cb = (r & s) != 0, (c & s) != 0
        w = jnp.where(rb == cb, w, jnp.where(cb, up, down))
    return w


def body(cfg, *refs):
    n, nimg, tok, d, heads, hd, ff, patch, chans = cfg
    (img_hbm, wp_hbm, bp_h, pos_h, g1_h, be1_h, wqkv_hbm, bqkv_h, wo_hbm, bo_h, g2_h, be2_h, w1_hbm, b1_h, w2_hbm, b2_h, out_hbm, out,
     img, wp_raw, wp, wq, wo, w1s, w1t, w2, bp, pos, g1, be1, bqkv, bo, g2, be2, b1, b2,
     zf, xs, x0, y1, yrecv, qkv, sbuf, pbuf, bsc, bcol, osend, orecv, res, y2, hid,
     outsem, isem, wsem, psem, qsem, csem, vsem, ssem, rsem, fsem, frsem, ossem, orsem) = refs
    ntok = n * tok
    gh, ng = 4, 3
    step, slots = w1s.shape[1], w1s.shape[0]
    gw = gh * hd
    me = lax.axis_index('sp')
    chip, core = me // 2, lax.rem(me, 2)
    pair, side = chip // 2, lax.rem(chip, 2)
    nxt = lax.rem(me + 1, n)
    pos_split, pos_full = pair, 2 + chip
    order = [i for i in range(nimg) if i % 3 == 1] + [i for i in range(nimg) if i % 3 != 1]

    def source_of(p, hg):
        return 2 * (2 * p + hg // 2) + 1 if p < 2 else 2 * (p - 2) + (hg == 0)

    def send_y(i, src_row, e, slot):
        return pltpu.make_async_remote_copy(
            y1.at[pl.ds(src_row, tok)], yrecv.at[0, pl.ds(pl.multiple_of(tok * slot, tok), tok)],
            ssem.at[i], rsem.at[slot], device_id={'sp': e}, device_id_type=MESH)

    def wait_sent(bi):
        for here in range(2):
            rows = pl.ds(0, tok * (n // 2 - (here != bi)))

            @pl.when(core == here)
            def _():
                pltpu.make_async_remote_copy(
                    yrecv.at[0, rows], yrecv.at[1, rows], ssem.at[bi], rsem.at[0], device_id={'sp': nxt}, device_id_type=MESH).wait_send()

    def forward(s, dst):
        rows = pl.ds(pl.multiple_of(tok * s, tok), tok)
        return pltpu.make_async_remote_copy(
            yrecv.at[0, rows], yrecv.at[1, rows], fsem.at[0], frsem.at[0], device_id={'sp': dst}, device_id_type=MESH)

    def forward_all(dst):
        return pltpu.make_async_remote_copy(
            yrecv.at[0], yrecv.at[1], fsem.at[0], frsem.at[0], device_id={'sp': dst}, device_id_type=MESH)

    def wave_of(g):
        return 1 - core if g < 2 else 1

    def send_o(g, s, hg, i):
        return pltpu.make_async_remote_copy(
            osend.at[g, pl.ds(pl.multiple_of(tok * s, tok), tok)], orecv.at[hg, pl.ds(pl.multiple_of(tok * i, tok), tok)],
            ossem.at[g], orsem.at[hg, wave_of(g)], device_id={'sp': s}, device_id_type=MESH)

    def head_group(g):
        return (1 - core) * (g + 1) + core * (2 * side + g) if g < 2 else (1 - core) * (g + 1)

    def w1_copy(c, slot, size):
        start = c * step if isinstance(c, int) else pl.multiple_of(c * step, step)
        return pltpu.make_async_copy(w1_hbm.at[pl.ds(start, size)], w1s.at[slot, pl.ds(0, size)], csem.at[slot])

    batches = (order[:2], order[2:])
    bounds = (0, 2, nimg)
    cp_img = [pltpu.make_async_copy(img_hbm.at[i], img.at[i], isem.at[0 if i in order[:2] else 1]) for i in range(nimg)]
    cp_wp = [pltpu.make_async_copy(wp_hbm.at[pl.ds(k, 2)], wp_raw.at[pl.ds(k, 2)], psem.at[0]) for k in range(0, patch, 2)]
    cp_wo = pltpu.make_async_copy(wo_hbm, wo, wsem.at[0])
    cp_w2 = pltpu.make_async_copy(w2_hbm, w2, wsem.at[1])
    cp_q = [pltpu.make_async_copy(
        wqkv_hbm.at[pl.ds(pl.multiple_of(d * t + gw * head_group(g), 32), gw)], wq.at[g, pl.ds(gw * t, gw)], qsem.at[g])
        for g in range(ng) for t in range(3)]
    cp_v = [pltpu.make_async_copy(a, b, vsem.at[k]) for k, (a, b) in enumerate(
        ((bp_h, bp), (pos_h, pos), (g1_h, g1), (be1_h, be1), (bqkv_h, bqkv), (bo_h, bo), (g2_h, g2), (be2_h, be2), (b1_h, b1), (b2_h, b2)))]
    for c in cp_wp + [cp_img[i] for i in batches[0]] + cp_v[:4] + [cp_img[i] for i in batches[1]] + cp_v[4:]:
        c.start()
    wp[...] = jnp.zeros_like(wp)
    barrier = pltpu.get_barrier_semaphore()
    for k in range(1, n):
        pl.semaphore_signal(barrier, inc=1, device_id={'sp': lax.rem(me + k, n)}, device_id_type=MESH)

    zf[...] = jnp.zeros_like(zf)
    lrow = lax.broadcasted_iota(jnp.int32, (224, 256), 0)
    lcol = lax.broadcasted_iota(jnp.int32, (224, 256), 1)
    sel = jnp.where((lcol % 16 < patch) & (lrow == patch * (lcol // 16) + lcol % 16), 1.0, 0.0).astype(BF16)

    full, early = ff // step, 3
    rest = ff - full * step

    def turn(c, size, slot):
        w1t[:, pl.ds(c * step if isinstance(c, int) else pl.multiple_of(c * step, step), size)] = jnp.transpose(w1s[slot, 0:size])

    def turn_step(c, carry):
        slot = lax.rem(c, slots)
        w1_copy(c, slot, step).wait()
        turn(c, step, slot)

        @pl.when(c + slots < full)
        def _():
            w1_copy(c + slots, slot, step).start()

        @pl.when(c + slots == full)
        def _():
            w1_copy(full, slot, rest).start()

        return carry

    for bi, batch in enumerate(batches):
        nb = len(batch)
        pltpu.make_async_copy(img_hbm.at[pl.ds(0, nb)], img.at[pl.ds(0, nb)], isem.at[bi]).wait()
        if bi == len(batches) - 1:
            for c in cp_q:
                c.start()
        for b, i in enumerate(batch):
            for y in range(2):
                for c in range(chans):
                    zf[(b * 2 + y) * chans + c, 0:patch, :] = img[i, c, patch * y:patch * y + patch, :]
        nz = nb * 2 * chans
        u = dot(zf[0:nz].reshape(nz * 16, 224).astype(BF16), sel)
        u = u.reshape(nz, 2, 8, 256)
        for ph in range(2):
            parts = []
            for xh in range(2):
                blk = u[:, ph, :, 128 * xh:128 * xh + 128].reshape(nz * 8, 128)
                parts.append(chunk_transpose(blk, 16).reshape(nz, 1, 8, 128))
            t = jnp.concatenate(parts, axis=1).reshape(nb * 2, chans, 16, 128).astype(BF16)
            for c in range(chans):
                xs[0:nb * tok, 256 * c + 128 * ph:256 * c + 128 * ph + 128] = t[:, c].reshape(nb * tok, 128)
        if bi == 0:
            pltpu.make_async_copy(wp_hbm, wp_raw, psem.at[0]).wait()
            for c in cp_v[:4]:
                c.wait()
            for c in range(slots):
                w1_copy(c, c, step).start()
            for c in range(chans):
                for p in range(patch):
                    wp[c, p, 0:patch, :] = wp_raw[p, c]
        e = dot(xs[0:nb * tok, :], wp[...].reshape(chans * 256, d))
        base = row(bp) + pos[...].astype(F32)
        xb = (e + jnp.concatenate([base] * nb, axis=0)).astype(BF16)
        yb = norm(xb.astype(F32), row(g1), row(be1)).astype(BF16)
        x0[tok * bounds[bi]:tok * bounds[bi + 1], :] = xb
        y1[tok * bounds[bi]:tok * bounds[bi + 1], :] = yb
        if bi == 0:
            pl.semaphore_wait(barrier, n - 1)
        if bi == 1:
            lax.fori_loop(0, early, turn_step, 0)
        for k in (2, 1, 3, 0):
            c = lax.rem(chip + k, n // 2)
            if bi == 0:
                e, p = 2 * c + 1, c // 2
            else:
                e, p = 2 * c, 2 + c
            src = pl.multiple_of(tok * p, tok)

            @pl.when(me != e)
            def _():
                send_y(bi, src, e, me).start()

            @pl.when(me == e)
            def _():
                yrecv[0, pl.ds(pl.multiple_of(tok * me, tok), tok), :] = y1[pl.ds(src, tok), :]

    for c in cp_v[4:]:
        c.wait()
    for t in range(3):
        for hg in range(heads // gh):
            bsc[t, hg, 0:gh, :] = bqkv[t, gh * hg:gh * hg + gh, :]
    for g in range(ng):
        for t in range(3):
            col = jnp.transpose(bsc[t, head_group(g)])
            for j in range(gh):
                bcol[g, gw * t + hd * j:gw * t + hd * j + hd, :] = jnp.broadcast_to(col[:, j:j + 1], (hd, 128))
    res[...] = x0[...].astype(F32) + row(bo)
    lax.fori_loop(early, full, turn_step, 0)

    cp_wo.start()
    cp_w2.start()
    w1_copy(full, full % slots, rest).wait()
    turn(full, rest, full % slots)

    def project(g, slot, parts):
        for t in parts:
            qkv[g % 2, gw * t:gw * t + gw, :] = dot(wq[g, gw * t:gw * t + gw, :], yrecv[slot], NT)

    def head(g, t, j):
        part = slice(gw * t + hd * j, gw * t + hd * j + hd)
        return qkv[g % 2, part, :] + jnp.concatenate([bcol[g, part, :]] * (ntok // 128), axis=1)

    def scores(g, j):
        sbuf[g % 2, j] = dot(jnp.transpose(head(g, 1, j)).astype(BF16), head(g, 0, j).astype(BF16))

    def soft(g, j):
        for b in range(0, ntok, 128):
            s = sbuf[g % 2, j, :, b:b + 128]
            p = jnp.exp2((s - jnp.max(s, axis=0, keepdims=True)) * (hd ** -0.5 * LOG2E))
            pbuf[g % 2, j, :, b:b + 128] = (p * (1.0 / jnp.sum(p, axis=0, keepdims=True))).astype(BF16)

    def mix(g, j):
        return dot(head(g, 2, j).astype(BF16), pbuf[g % 2, j])

    def wait_q(g):
        pltpu.make_async_copy(wqkv_hbm.at[pl.ds(0, 3 * gw)], wq.at[g], qsem.at[g]).wait()

    def run_groups(gs, slot, i):
        for g in gs:
            wait_q(g)
        project(gs[0], slot, range(3))
        for g in gs:
            for j in range(gh):
                scores(g, j)
            outs = []
            for j in range(gh):
                if g + 1 in gs and j < 3:
                    project(g + 1, slot, (j,))
                soft(g, j)
                if j:
                    outs.append(mix(g, j - 1))
            outs.append(mix(g, gh - 1))
            osend[g] = jnp.transpose(jnp.concatenate(outs, axis=0)).astype(BF16)
            hg = head_group(g)
            for k in (4, 5, 3, 2, 6, 7, 1):
                send_o(g, lax.rem(me + k, n), hg, i).start()
            orecv[hg, pl.ds(pl.multiple_of(tok * i, tok), tok), :] = osend[g, pl.ds(pl.multiple_of(tok * me, tok), tok), :]


    @pl.when(core == 0)
    def _():
        for k in (0, 1, 2, 3, 6, 7, 4, 5):
            s = lax.rem(me + k, n)
            if k:
                send_y(0, 0, s, s).wait_recv()
            forward(s, me + 1).start()
        run_groups((0, 1, 2), 0, pos_full)

    @pl.when(core == 1)
    def _():
        for k in range(1, n):
            s = lax.rem(me + k, n)
            send_y(0, 0, s, s).wait_recv()
        run_groups((0, 1), 0, pos_split)
        forward_all(me - 1).wait_recv()
        run_groups((2,), 1, pos_full)

    cp_wo.wait()
    cp_w2.wait()
    def recv_o(w, hg):
        lo, hi = bounds[w], bounds[w + 1]
        mine = sum(jnp.where(me == source_of(p, hg), 1, 0) for p in range(lo, hi))
        for k in range(2):
            got = pl.ds(0, tok * (hi - lo - k))

            @pl.when(mine == k)
            def _():
                pltpu.make_async_remote_copy(
                    osend.at[0, got], orecv.at[hg, got], ossem.at[0], orsem.at[hg, w],
                    device_id={'sp': nxt}, device_id_type=MESH).wait_recv()

    def join(w, hgs):
        rows = slice(tok * bounds[w], tok * bounds[w + 1])
        o = jnp.concatenate([orecv[hg, rows, :] for hg in hgs], axis=1)
        res[rows, :] += dot(o, wo[...])

    def expand(w):
        rows = slice(tok * bounds[w], tok * bounds[w + 1])
        y2[rows, :] = norm(res[rows, :], row(g2), row(be2)).astype(BF16)
        for c in range(0, ff, 512):
            k = min(512, ff - c)
            h = dot(y2[rows, :], w1t[:, c:c + k]) + b1[pl.ds(c, k)].reshape(1, k)
            hid[rows, c:c + k] = gelu(h).astype(BF16)

    def contract(w):
        lo, hi = bounds[w], bounds[w + 1]
        rows = slice(tok * lo, tok * hi)
        for j in range(0, d, 256):
            k = min(256, d - j)
            acc = res[rows, j:j + k] + dot(hid[rows, :], w2[:, j:j + k])
            acc = (acc + b2[pl.ds(j, k)].reshape(1, k)).astype(BF16)
            for p in range(lo, hi):
                out[tok * order[p]:tok * order[p] + tok, j:j + k] = acc[tok * (p - lo):tok * (p - lo) + tok, :]
            if w == 1:
                pltpu.make_async_copy(out.at[:, pl.ds(j, k)], out_hbm.at[:, pl.ds(j, k)], outsem.at[0]).start()

    for w in range(2):
        for hg in ((0, 2, 1, 3), (1, 0, 2, 3))[w]:
            recv_o(w, hg)
        join(w, range(4))
        expand(w)
        contract(w)
    wait_sent(0)
    wait_sent(1)

    @pl.when(core == 0)
    def _():
        forward_all(me + 1).wait_send()

    def drain(gs):
        rows = pl.ds(0, tok * (n - 1))
        for g in gs:
            pltpu.make_async_remote_copy(
                osend.at[g, rows], osend.at[0, rows], ossem.at[g], orsem.at[0, 0], device_id={'sp': nxt}, device_id_type=MESH).wait_send()

    drain(range(ng))

    pltpu.make_async_copy(out, out_hbm, outsem.at[0]).wait()


def solution(mesh):
    n = mesh.shape['sp']

    def device_step(images, w_patch, b_patch, pos_embed, ln1_gain, ln1_bias, w_qkv, b_qkv, w_out, b_out, ln2_gain, ln2_bias, w_fc1, b_fc1, w_fc2, b_fc2):
        nimg, rows, width, chans = images.shape
        tok, d = pos_embed.shape
        patch = w_patch.shape[0]
        _, _, heads, hd = w_qkv.shape
        ff = w_fc1.shape[1]
        m = nimg * tok
        ntok = n * tok
        cfg = (n, nimg, tok, d, heads, hd, ff, patch, chans)
        img_t = jnp.transpose(images, (0, 3, 1, 2))
        wp_t = jnp.transpose(w_patch, (0, 2, 1, 3))
        wqkv_t = jnp.transpose(w_qkv, (1, 2, 3, 0)).reshape(3 * d, d)
        wo_t = w_out.reshape(d, d)
        w1_t = jnp.transpose(w_fc1, (1, 0))

        hbm = pl.BlockSpec(memory_space=pltpu.HBM)
        V, S = pltpu.VMEM, pltpu.SemaphoreType.DMA
        out = pl.pallas_call(
            functools.partial(body, cfg),
            out_shape=jax.ShapeDtypeStruct((m, d), BF16),
            in_specs=[hbm] * 16,
            out_specs=hbm,
            scratch_shapes=[
                V((m, d), BF16),
                V(img_t.shape, F32), V(wp_t.shape, BF16), V((chans, 16, 16, d), BF16),
                V((3, 12 * hd, d), BF16), V((d, d), BF16), V((4, 512, d), BF16), V((d, ff), BF16), V((ff, d), BF16),
                V((d,), F32), V((tok, d), BF16), V((d,), F32), V((d,), F32), V((3, heads, hd), F32), V((d,), F32), V((d,), F32),
                V((d,), F32), V((ff,), F32), V((d,), F32),
                V((8 * chans, 16, width), F32), V((4 * tok, chans * 256), BF16),
                V((m, d), BF16), V((m, d), BF16), V((2, ntok, d), BF16),
                V((2, 12 * hd, ntok), F32), V((2, 4, ntok, ntok), F32), V((2, 4, ntok, ntok), BF16),
                V((3, 4, 8, hd), F32), V((3, 12 * hd, 128), F32),
                V((3, ntok, 4 * hd), BF16), V((4, m, 4 * hd), BF16), V((m, d), F32), V((m, d), BF16), V((m, ff), BF16),
                S((1,)), S((2,)), S((2,)), S((1,)), S((3,)), S((4,)), S((10,)), S((2,)), S((n,)), S((1,)), S((1,)), S((3,)), S((4, 2)),
            ],
            compiler_params=pltpu.CompilerParams(collective_id=0, has_side_effects=True, vmem_limit_bytes=60 * 1024 * 1024),
            name='siglip_layer',
        )(img_t, wp_t, b_patch, pos_embed, ln1_gain, ln1_bias, wqkv_t, b_qkv, wo_t, b_out,
          ln2_gain, ln2_bias, w1_t, b_fc1, w_fc2, b_fc2)
        return out.reshape(nimg, tok, d)

    in_specs = (P('dp', 'sp', None, None), P(), P(), P('sp', None), P(), P(), P(), P(), P(), P(), P(), P(), P(), P(), P(), P())
    return jax.shard_map(device_step, mesh=mesh, in_specs=in_specs, out_specs=P('dp', 'sp', None), check_vma=False)
```
